32 devices in a mesh: scen: 8 (over y, x, core), col: 4 (over z).
Axes of the slice: x: 2, y: 2, z: 4, core: 2. Of those that a mesh axis runs over, the one named last changes fastest.
Arguments:
- coef: float32 [4096, 8192], P('scen', 'col'), as said below
- mask: int32 [4096], replicated, may hold values from 0 to 1, as said below
- assign: int32 [512], replicated, may hold values from 0 to 511, each once
Outputs:
- master: float32 [4, 2048, 4096], P('col', 'scen')
The draws below stay inside these ranges and needn't reach their ends.
Inputs may be any that keep to these rules, and one draw needn't show every extreme that they name: `mask`: in each aligned block of 512 cuts (the cuts of one index of scen) exactly 256 are active. `coef`: magnitudes of rows and of columns differ widely; entries are finite and not zero on every row.
All inputs are finite; a program needn't handle non-finite values.
Results may differ from the reference program's by a relative error of at most 0.00007.
Values sent between devices are 32-bit elements; how exact they have to be, the bound alone decides.
No kernel may reach another device: no remote copies, remote signals or barrier semaphores. Data moves between devices by JAX's collectives and lax.ppermute only.
A program may use at most 128 MiB of HBM per device.

```python
import jax
import jax.numpy as jnp
from jax import lax

NV = 8192
K = 8
SCEN_DEV = 64
ROWS_DEV = 512
ACT_DEV = 256
SCEN = 512
CUTS = 4096
GROUPS = 4
N_SCEN = 8


def draw_coef(key, part):
    keys = jax.random.split(jax.random.fold_in(key, 11), 3)
    ramp = 1.0 + 2.0 * jnp.arange(NV, dtype=jnp.float32) / NV
    base = jax.random.normal(keys[0], (CUTS, NV), jnp.float32)
    row_scale = jnp.exp(jax.random.uniform(keys[1], (CUTS, 1), jnp.float32, -2.3, 2.3))
    col_scale = jnp.exp(jax.random.uniform(keys[2], (1, NV), jnp.float32, -2.3, 2.3)) * ramp[None, :]
    return (base * row_scale * col_scale).astype(jnp.float32)


def draw_mask(key, part):
    blocks = SCEN // SCEN_DEV
    keys = jax.random.split(jax.random.fold_in(key, 23), blocks)
    orders = jax.vmap(lambda sub: jax.random.permutation(sub, ROWS_DEV))(keys)
    return (orders < ACT_DEV).astype(jnp.int32).reshape(CUTS)


def setup_inputs(seed: int = 0) -> dict:
    streams_of = jax.random.split(jax.random.key(seed), 4)
    return {
        "coef": draw_coef(jax.random.fold_in(streams_of[3], 71), 0),
        "mask": draw_mask(jax.random.fold_in(streams_of[3], 71), 0),
        "assign": jax.random.permutation(streams_of[2], SCEN).astype(jnp.int32),
    }


EPS = 1e-06

def reference(coef, mask, assign):
    total = lax.optimization_barrier(jnp.sum(coef * coef, axis=1))
    row_norm = jnp.sqrt(total / NV + EPS)
    live = mask.astype(jnp.float32)
    scaled = coef / row_norm[:, None] * live[:, None]
    column = lax.optimization_barrier(jnp.sum(scaled * scaled, axis=0))
    col_norm = jnp.sqrt(column / (ACT_DEV * N_SCEN) + EPS)
    equil = scaled / col_norm[None, :]
    inverse = jnp.argsort(assign, stable=True).astype(jnp.int32)
    position = jnp.arange(CUTS, dtype=jnp.int32)
    source = inverse[position // K] * K + position % K
    master = jnp.take(equil, source, axis=0).T
    return master.reshape(GROUPS, NV // GROUPS, CUTS)
```

```python
import functools

import jax
import jax.numpy as jnp
from jax import lax
from jax.experimental import pallas as pl
from jax.experimental.pallas import tpu as pltpu
from jax.sharding import PartitionSpec as P

NV = 8192
K = 8
ACT_DEV = 256


EPS = 1e-06
LANES = 128
SUBLANES = 8
CHUNKS = 4
VMEM = pl.BlockSpec(memory_space=pltpu.VMEM)
SMEM = pl.BlockSpec(memory_space=pltpu.SMEM)
HBM = pl.BlockSpec(memory_space=pltpu.HBM)
PARAMS = pltpu.CompilerParams(vmem_limit_bytes=24 * 1024 * 1024)


def pick_kernel(groups, rows, slice_width, mask_ref, coef_ref, *refs):
    outs = refs[:groups]
    part_ref, coef_v, squares, live, order, sems, mask_sem = refs[groups:]
    me = lax.axis_index("scen")
    tiles = slice_width // LANES
    chunk = rows // CHUNKS

    def copy(c, k, h):
        span = pl.ds(c * chunk, chunk)
        column = pl.multiple_of((jnp.bitwise_xor(me, k) * tiles + h) * LANES, LANES)
        t = k * tiles + h
        return pltpu.make_async_copy(
            coef_ref.at[span, pl.ds(column, LANES)], coef_v.at[t, span], sems.at[c, t]
        )

    places = [(k, h) for k in range(groups) for h in range(tiles)]
    mask_copy = pltpu.make_async_copy(mask_ref.at[pl.ds(me * rows, rows)], live, mask_sem)
    mask_copy.start()
    for c in range(CHUNKS):
        for k, h in places:
            copy(c, k, h).start()
    lane_row = lax.broadcasted_iota(jnp.int32, (SUBLANES, LANES), 0)

    def note(i, n):
        marks = [live[i * SUBLANES + j] for j in range(SUBLANES)]
        for j in range(SUBLANES):
            order[n] = i * SUBLANES + j
            n = n + marks[j]
        return n

    def gather(i, carry):
        first = pl.multiple_of(i * SUBLANES, SUBLANES)
        picks = [order[first + j] for j in range(SUBLANES)]
        total = jnp.zeros((SUBLANES, LANES), jnp.float32)
        for k, h in places:
            t = k * tiles + h
            tile = coef_v[t, pl.ds(picks[0], SUBLANES, stride=0), :]
            for j in range(1, SUBLANES):
                line = coef_v[t, pl.ds(picks[j], SUBLANES, stride=0), :]
                tile = jnp.where(lane_row == j, line, tile)
            outs[k][pl.ds(first, SUBLANES), h * LANES : (h + 1) * LANES] = tile
            total = total + tile * tile
        squares[pl.ds(first, SUBLANES), :] = total
        return carry

    mask_copy.wait()
    found = jnp.int32(0)
    ends = []
    for c in range(CHUNKS):
        found = lax.fori_loop(
            c * chunk // SUBLANES, (c + 1) * chunk // SUBLANES, note, found, unroll=2
        )
        ends.append(found // SUBLANES)
    done = jnp.int32(0)
    for c in range(CHUNKS):
        for k, h in places:
            copy(c, k, h).wait()
        lax.fori_loop(done, ends[c], gather, 0)
        done = ends[c]
    part_ref[...] = lax.dot_general(
        jnp.ones((SUBLANES, LANES), jnp.float32), squares[...],
        (((1,), (1,)), ((), ())),
        precision=lax.Precision.HIGHEST, preferred_element_type=jnp.float32,
    )


def pick(mask, coef, groups, rows, slice_width):
    block = pltpu.VMEM((ACT_DEV, slice_width), jnp.float32)
    tiles = groups * slice_width // LANES
    return pl.pallas_call(
        functools.partial(pick_kernel, groups, rows, slice_width),
        out_shape=[block] * groups + [pltpu.VMEM((SUBLANES, ACT_DEV), jnp.float32)],
        in_specs=[HBM, HBM],
        out_specs=[VMEM] * (groups + 1),
        scratch_shapes=[
            pltpu.VMEM((tiles, rows, LANES), jnp.float32),
            pltpu.VMEM((ACT_DEV, LANES), jnp.float32),
            pltpu.SMEM((rows,), jnp.int32),
            pltpu.SMEM((ACT_DEV + SUBLANES,), jnp.int32),
            pltpu.SemaphoreType.DMA((CHUNKS, tiles)),
            pltpu.SemaphoreType.DMA,
        ],
        name="pick",
        compiler_params=PARAMS,
    )(*[pltpu.with_memory_space_constraint(value, pltpu.HBM) for value in (mask, coef)])


def spread_kernel(groups, rows, mask_ref, place_ref):
    live = mask_ref[...]
    before = lax.broadcasted_iota(jnp.int32, (rows, rows), 0) < lax.broadcasted_iota(
        jnp.int32, (rows, rows), 1
    )
    rank = jnp.dot(
        live.astype(jnp.float32).astype(jnp.bfloat16),
        before.astype(jnp.float32).astype(jnp.bfloat16),
        preferred_element_type=jnp.float32,
    )
    key = jnp.where(live > 0, rank, -1.0).T
    packed = lax.broadcasted_iota(jnp.int32, (rows, ACT_DEV), 1).astype(jnp.float32)
    for s in range(groups):
        hit = key[:, s : s + 1] == packed
        place_ref[s] = jnp.where(hit, 1.0, 0.0).astype(jnp.bfloat16)


def spread(mask, groups, rows):
    return pl.pallas_call(
        functools.partial(spread_kernel, groups, rows),
        out_shape=pltpu.VMEM((groups, rows, ACT_DEV), jnp.bfloat16),
        in_specs=[VMEM],
        out_specs=VMEM,
        name="spread",
        compiler_params=PARAMS,
    )(mask.reshape(groups, rows))


def inverse_norms(totals):
    total = totals[0][...]
    for other in totals[1:]:
        total = total + other[...]
    return (1.0 / jnp.sqrt(total / NV + EPS)).T


def put(k, scale, got_ref, place_ref, assign_ref, flat_ref, wide):
    rows = wide.shape[0]
    slots = rows // K
    source = jnp.bitwise_xor(lax.axis_index("scen"), k)
    value = got_ref[...] * scale
    squares = jnp.sum((value * value).reshape(ACT_DEV // SUBLANES, SUBLANES, -1), axis=0)
    high = value.astype(jnp.bfloat16)
    low = (value - high.astype(jnp.float32)).astype(jnp.bfloat16)
    place = place_ref[source]
    wide[...] = jnp.dot(place, high, preferred_element_type=jnp.float32) + jnp.dot(
        place, low, preferred_element_type=jnp.float32
    )
    for i in range(slots):
        at = pl.multiple_of(assign_ref[source * slots + i] * K, K)
        flat_ref[pl.ds(at, K), :] = wide[i * K : (i + 1) * K, :]
    return squares


def early_kernel(lines, assign_ref, place_ref, *refs):
    n = len(lines)
    totals, got = refs[:4], refs[4 : 4 + n]
    flat_ref, squares_ref, wide = refs[4 + n :]
    scale = inverse_norms(totals)
    squares = None
    for (k, line), got_ref in zip(lines, got):
        one = put(k, scale[:, line : line + 1], got_ref, place_ref, assign_ref, flat_ref, wide)
        squares = one if squares is None else squares + one
    squares_ref[...] = squares


def late_kernel(lines, active_total, assign_ref, place_ref, *refs):
    n = len(lines)
    totals, got = refs[:4], refs[4 : 4 + n]
    flat_ref, squares_ref, out_ref, wide, out_v, sems = refs[4 + n :]
    scale = inverse_norms(totals)
    squares = squares_ref[...]
    for (k, line), got_ref in zip(lines, got):
        squares = squares + put(
            k, scale[:, line : line + 1], got_ref, place_ref, assign_ref, flat_ref, wide
        )
    column = jnp.sum(squares, axis=0, keepdims=True)
    inverse = 1.0 / jnp.sqrt(column / active_total + EPS)
    cuts = flat_ref.shape[0]
    step = 4 * LANES
    copies = []
    for c in range(cuts // step):
        span = pl.ds(c * step, step)
        out_v[:, span] = (flat_ref[span, :] * inverse).T
        copies.append(pltpu.make_async_copy(out_v.at[:, span], out_ref.at[0, :, span], sems.at[c]))
        copies[-1].start()
    for one in copies:
        one.wait()


def on_chip(value):
    return pltpu.with_memory_space_constraint(value, pltpu.VMEM)


def finish(received, lines_of, last, totals, place, assign, groups, rows, slice_width):
    received = {k: on_chip(v) for k, v in received.items()}
    totals = [on_chip(v) for v in totals]
    cuts = groups * rows
    flat = pltpu.VMEM((cuts, slice_width), jnp.float32)
    squares = pltpu.VMEM((SUBLANES, slice_width), jnp.float32)
    wide = pltpu.VMEM((rows, slice_width), jnp.float32)
    early = [k for k in range(groups) if k not in last]
    flat, squares = pl.pallas_call(
        functools.partial(early_kernel, [(k, lines_of[k]) for k in early]),
        out_shape=[flat, squares],
        in_specs=[SMEM] + [VMEM] * (1 + len(totals) + len(early)),
        out_specs=[VMEM, VMEM],
        scratch_shapes=[wide],
        name="early",
        compiler_params=PARAMS,
    )(assign, place, *totals, *[received[k] for k in early])
    return pl.pallas_call(
        functools.partial(late_kernel, [(k, lines_of[k]) for k in last], ACT_DEV * groups),
        out_shape=jax.ShapeDtypeStruct((1, slice_width, cuts), jnp.float32),
        in_specs=[SMEM] + [VMEM] * (3 + len(totals) + len(last)),
        out_specs=HBM,
        scratch_shapes=[
            wide,
            pltpu.VMEM((slice_width, cuts), jnp.float32),
            pltpu.SemaphoreType.DMA((cuts // (4 * LANES),)),
        ],
        name="late",
        compiler_params=PARAMS,
    )(assign, place, *totals, *[received[k] for k in last], flat, squares)


def send_order(groups):
    return [k for k in range(2, groups, 2)] + [k for k in range(1, groups, 2)][::-1]


def exchange(coef, mask, assign):
    rows, width = coef.shape
    groups = lax.axis_size("scen")
    columns = lax.axis_size("col")
    slice_width = width // groups

    def swap(value, k):
        return lax.ppermute(value, "scen", [(i, i ^ k) for i in range(groups)])

    *blocks, part = pick(mask, coef, groups, rows, slice_width)
    received = {0: blocks[0]}
    sends = send_order(groups)
    for k in sends[:2]:
        received[k] = swap(blocks[k], k)
    evens = [k for k in range(0, groups, 2)]
    parts = [part[:1]] + [swap(part, k)[:1] for k in evens[1:]]
    for k in sends[2:]:
        received[k] = swap(blocks[k], k)
    half = jnp.concatenate(parts, axis=0)
    other = swap(half, 1)
    lines = jnp.concatenate([half, other], axis=0)
    lines_of = {k: n for n, k in enumerate(evens + [k ^ 1 for k in evens])}
    totals = [lines] + [
        lax.ppermute(lines, "col", [(i, (i + z) % columns) for i in range(columns)])
        for z in range(1, columns)
    ]
    place = spread(mask, groups, rows)
    return finish(received, lines_of, [sends[-2]], totals, place, assign, groups, rows, slice_width)


def fallback(coef, mask, assign):
    rows, width = coef.shape
    groups = lax.axis_size("scen")
    slice_width = width // groups
    cut_total = groups * rows
    slot_total = cut_total // K
    active_total = ACT_DEV * groups
    partial_value = jnp.sum(coef * coef, axis=1)
    total = lax.psum(partial_value, "col")
    row_norm = jnp.sqrt(total / NV + EPS)
    device_index = lax.axis_index("scen")
    own_mask = lax.dynamic_slice_in_dim(mask, device_index * rows, rows)
    live = own_mask.astype(jnp.float32)
    scaled = coef / row_norm[:, None] * live[:, None]
    flipped = scaled.T.reshape(groups, slice_width, rows)
    inverse = jnp.argsort(assign, stable=True)
    kept_rows = jnp.argsort(1 - own_mask, stable=True)[:ACT_DEV]
    picked = jnp.take(flipped, kept_rows, axis=2)
    arrived = lax.all_to_all(picked, "scen", split_axis=0, concat_axis=2, tiled=True)
    norm = jnp.sqrt(jnp.sum(arrived * arrived, axis=2, keepdims=True) / active_total + EPS)
    equil = (arrived / norm).reshape(slice_width, groups, ACT_DEV)
    block_masks = mask.reshape(groups, rows)
    chosen = jnp.argsort(1 - block_masks, axis=1, stable=True)[:, :ACT_DEV]
    bundle = min(groups, 8)
    rounds = groups // bundle
    chosen_sets = chosen.reshape(rounds, bundle, ACT_DEV)
    equil_sets = equil.reshape(slice_width, rounds, bundle, ACT_DEV).transpose(1, 0, 2, 3)
    local_rows = jnp.arange(rows, dtype=jnp.int32)

    def place(pair):
        chosen_set, equil_set = pair
        placing = (chosen_set[:, :, None] == local_rows[None, None, :]).astype(jnp.float32)
        return jnp.einsum("sga,gar->sgr", equil_set, placing, precision=lax.Precision.HIGHEST)

    placed = lax.map(place, (chosen_sets, equil_sets))
    whole = placed.transpose(1, 0, 2, 3).reshape(1, slice_width, cut_total)
    slotted = whole.reshape(1, slice_width, slot_total, K)
    return jnp.take(slotted, inverse, axis=2).reshape(1, slice_width, cut_total)


def solution(mesh):
    in_specs = (P("scen", "col"), P(), P())
    out_specs = P("col", "scen", None)
    groups, columns = mesh.shape["scen"], mesh.shape["col"]
    paired = groups >= 4 and groups & (groups - 1) == 0
    fits = NV % (groups * columns * LANES) == 0
    shard = functools.partial(
        jax.shard_map, mesh=mesh, in_specs=in_specs, out_specs=out_specs, check_vma=False
    )
    if not (paired and fits):
        return shard(fallback)
    return shard(exchange)
```

```python
import functools

import jax
import jax.numpy as jnp
from jax import lax
from jax.experimental import pallas as pl
from jax.experimental.pallas import tpu as pltpu
from jax.sharding import PartitionSpec as P

NV = 8192
K = 8
ACT_DEV = 256


EPS = 1e-06
LANES = 128
SUBLANES = 8
CHUNKS = 4
VMEM = pl.BlockSpec(memory_space=pltpu.VMEM)
HBM = pl.BlockSpec(memory_space=pltpu.HBM)
SMEM = pl.BlockSpec(memory_space=pltpu.SMEM)
PARAMS = pltpu.CompilerParams(vmem_limit_bytes=16 * 1024 * 1024)


def on_chip(*values):
    return [pltpu.with_memory_space_constraint(value, pltpu.VMEM) for value in values]


def scalars(value):
    return pltpu.with_memory_space_constraint(value, pltpu.SMEM)


def in_hbm(*values):
    return [pltpu.with_memory_space_constraint(value, pltpu.HBM) for value in values]


def evens(groups):
    return list(range(0, groups, 2))


def odds(groups):
    return list(range(1, groups, 2))


def halved(groups):
    return odds(groups)[1:-1]


def pieces(groups, tiles):
    whole = [(k, 0, tiles) for k in range(groups) if k not in halved(groups)]
    first = [(k, 0, tiles // 2) for k in halved(groups)]
    second = [(k, tiles // 2, tiles) for k in halved(groups)]
    return whole + first + second


def pack(first, picks, window, cells, total):
    lane_row = lax.broadcasted_iota(jnp.int32, (SUBLANES, LANES), 0)
    for t, out, lane in cells:
        tile = window[t, pl.ds(picks[0], SUBLANES), :]
        for j in range(1, SUBLANES):
            tile = jnp.where(lane_row == j, window[t, pl.ds(picks[j], SUBLANES), :], tile)
        out[pl.ds(first, SUBLANES), lane : lane + LANES] = tile
        total = total + tile * tile
    return total


def cells_of(parts, outs, tiles):
    return [
        (k * tiles + h, out, (h - h0) * LANES)
        for (k, h0, h1), out in zip(parts, outs)
        for h in range(h0, h1)
    ]


def first_kernel(groups, rows, tiles, parts, mask_ref, coef_ref, *refs):
    outs = refs[: len(parts)]
    window, squares, order, live, sems, mask_sem = refs[len(parts) :]
    me = lax.axis_index("scen")
    chunk = rows // CHUNKS
    places = [(k, h) for k in range(groups) for h in range(tiles)]
    cells = cells_of(parts, outs, tiles)
    places.sort(key=lambda place: place[0] not in [k for k, _, _ in parts])

    def copy(c, k, h):
        span = pl.ds(c * chunk, chunk)
        column = pl.multiple_of((jnp.bitwise_xor(me, k) * tiles + h) * LANES, LANES)
        t = k * tiles + h
        return pltpu.make_async_copy(
            coef_ref.at[span, pl.ds(column, LANES)], window.at[t, span], sems.at[c, t]
        )

    mask_copy = pltpu.make_async_copy(mask_ref.at[pl.ds(me * rows, rows)], live, mask_sem)
    mask_copy.start()
    for k, h in places:
        for c in range(CHUNKS):
            copy(c, k, h).start()

    def note(i, n):
        marks = [live[i * SUBLANES + j] for j in range(SUBLANES)]
        for j in range(SUBLANES):
            order[n] = i * SUBLANES + j
            n = n + marks[j]
        return n

    def gather(i, carry):
        first = pl.multiple_of(i * SUBLANES, SUBLANES)
        picks = [order[first + j] - j for j in range(SUBLANES)]
        total = jnp.zeros((SUBLANES, LANES), jnp.float32)
        squares[pl.ds(first, SUBLANES), :] = pack(first, picks, window, cells, total)
        return carry

    mask_copy.wait()
    lax.fori_loop(0, rows // SUBLANES, note, jnp.int32(0), unroll=4)
    inside = [k for k, _, _ in parts]
    for k, h in places:
        for c in range(CHUNKS):
            if k in inside:
                copy(c, k, h).wait()
    lax.fori_loop(0, ACT_DEV // SUBLANES, gather, 0, unroll=2)
    for k, h in places:
        for c in range(CHUNKS):
            if k not in inside:
                copy(c, k, h).wait()


def second_kernel(tiles, parts, window, before, order, *refs):
    outs = refs[: len(parts)]
    part_ref, squares = refs[len(parts) :]
    cells = cells_of(parts, outs, tiles)

    def gather(i, carry):
        first = pl.multiple_of(i * SUBLANES, SUBLANES)
        picks = [order[first + j] - j for j in range(SUBLANES)]
        total = before[pl.ds(first, SUBLANES), :]
        squares[pl.ds(first, SUBLANES), :] = pack(first, picks, window, cells, total)
        return carry

    lax.fori_loop(0, ACT_DEV // SUBLANES, gather, 0)
    part_ref[...] = lax.dot_general(
        jnp.ones((SUBLANES, LANES), jnp.float32), squares[...],
        (((1,), (1,)), ((), ())),
        precision=lax.Precision.HIGHEST, preferred_element_type=jnp.float32,
    )


def pick(mask, coef, groups, rows, tiles):
    parts = pieces(groups, tiles)
    ahead = [part for part in parts if part[0] == evens(groups)[-1]]
    behind = [part for part in parts if part not in ahead]

    def blocks(some):
        room = {1: SUBLANES}
        return [
            pltpu.VMEM((ACT_DEV + room.get(k, 0), (h1 - h0) * LANES), jnp.float32)
            for k, h0, h1 in some
        ]

    squares = pltpu.VMEM((ACT_DEV, LANES), jnp.float32)
    window = pltpu.VMEM((groups * tiles, rows + SUBLANES, LANES), jnp.float32)
    *one, window, before, order = pl.pallas_call(
        functools.partial(first_kernel, groups, rows, tiles, ahead),
        out_shape=blocks(ahead) + [window, squares, pltpu.SMEM((rows,), jnp.int32)],
        in_specs=[HBM, HBM],
        out_specs=[VMEM] * (len(ahead) + 2) + [SMEM],
        scratch_shapes=[
            pltpu.SMEM((rows,), jnp.int32),
            pltpu.SemaphoreType.DMA((CHUNKS, groups * tiles)),
            pltpu.SemaphoreType.DMA,
        ],
        name="first",
        compiler_params=PARAMS,
    )(*in_hbm(mask, coef))
    *two, part = pl.pallas_call(
        functools.partial(second_kernel, tiles, behind),
        out_shape=blocks(behind) + [pltpu.VMEM((SUBLANES, ACT_DEV), jnp.float32)],
        in_specs=[VMEM, VMEM, SMEM],
        out_specs=[VMEM] * (len(behind) + 1),
        scratch_shapes=[squares],
        name="second",
        compiler_params=PARAMS,
    )(*on_chip(window, before), scalars(order))
    found = zip(ahead + behind, one + two)
    return {(k, h0): block for (k, h0, _), block in found}, part


def join_kernel(block_ref, *refs):
    out_ref = refs[-1]
    for n, ref in enumerate(refs[:-1]):
        out_ref[ACT_DEV + n : ACT_DEV + n + 1, :] = ref[:1, :]


def join(block, *values):
    return pl.pallas_call(
        join_kernel,
        out_shape=pltpu.VMEM(block.shape, jnp.float32),
        in_specs=[VMEM] * (1 + len(values)),
        out_specs=VMEM,
        input_output_aliases={0: 0},
        name="join",
        compiler_params=PARAMS,
    )(*on_chip(block, *values))


def stack_kernel(take, *refs):
    for n, ref in enumerate(refs[:-1]):
        refs[-1][n * take : (n + 1) * take, :] = ref[ACT_DEV : ACT_DEV + take, :]


def stack(take, *values):
    return pl.pallas_call(
        functools.partial(stack_kernel, take),
        out_shape=pltpu.VMEM((take * len(values), values[0].shape[1]), jnp.float32),
        in_specs=[VMEM] * len(values),
        out_specs=VMEM,
        name="stack",
        compiler_params=PARAMS,
    )(*on_chip(*values))


def spread_kernel(groups, rows, mask_ref, assign_ref, place_ref, slots_ref, sem):
    copy = pltpu.make_async_copy(assign_ref, slots_ref, sem)
    copy.start()
    lines = [mask_ref[pl.ds(s * rows, rows)].reshape(1, rows) for s in range(groups)]
    live = jnp.concatenate(lines, axis=0)
    before = lax.broadcasted_iota(jnp.int32, (rows, rows), 0) < lax.broadcasted_iota(
        jnp.int32, (rows, rows), 1
    )
    rank = jnp.dot(
        live.astype(jnp.float32).astype(jnp.bfloat16),
        before.astype(jnp.float32).astype(jnp.bfloat16),
        preferred_element_type=jnp.float32,
    )
    key = jnp.where(live > 0, rank, -1.0).T
    packed = lax.broadcasted_iota(jnp.int32, (rows, ACT_DEV), 1).astype(jnp.float32)
    for s in range(groups):
        hit = key[:, s : s + 1] == packed
        place_ref[s] = jnp.where(hit, 1.0, 0.0).astype(jnp.bfloat16)
    copy.wait()


def spread(mask, assign, groups, rows):
    place = pltpu.VMEM((groups, rows, ACT_DEV), jnp.bfloat16)
    return pl.pallas_call(
        functools.partial(spread_kernel, groups, rows),
        out_shape=[place, pltpu.SMEM(assign.shape, jnp.int32)],
        in_specs=[VMEM, HBM],
        out_specs=[VMEM, SMEM],
        scratch_shapes=[pltpu.SemaphoreType.DMA],
        name="spread",
        compiler_params=PARAMS,
    )(*on_chip(mask), *in_hbm(assign))


def inverse_norms(totals):
    total = totals[0][...]
    for other in totals[1:]:
        total = total + other[...]
    return (1.0 / jnp.sqrt(total / NV + EPS)).T


def place_rows(k, scale, got_ref, place_ref, assign_ref, flats):
    source = jnp.bitwise_xor(lax.axis_index("scen"), k)
    value = got_ref[:ACT_DEV, :] * scale
    high = value.astype(jnp.bfloat16)
    low = (value - high.astype(jnp.float32)).astype(jnp.bfloat16)
    place = place_ref[source]
    wide = jnp.dot(place, high, preferred_element_type=jnp.float32) + jnp.dot(
        place, low, preferred_element_type=jnp.float32
    )
    slots = wide.shape[0] // K
    for i in range(slots):
        at = pl.multiple_of(assign_ref[source * slots + i] * K, K)
        lane = 0
        for flat in flats:
            width = flat.shape[1]
            flat[pl.ds(at, K), :] = wide[i * K : (i + 1) * K, lane : lane + width]
            lane += width
    return jnp.sum((value * value).reshape(ACT_DEV // SUBLANES, SUBLANES, -1), axis=0)


def early_kernel(lines, rest, assign_ref, place_ref, *refs):
    n = len(lines)
    totals, got = refs[:4], refs[4 : 4 + n]
    outs = refs[4 + n :]
    flats, (squares_a, squares_b), scales = outs[:2], outs[2:4], outs[4:]
    scale = inverse_norms(totals)
    for line, ref in zip(rest, scales):
        ref[...] = jnp.broadcast_to(scale[:, line : line + 1], ref.shape)
    squares = None
    for (k, line), got_ref in zip(lines, got):
        one = place_rows(k, scale[:, line : line + 1], got_ref, place_ref, assign_ref, flats)
        squares = one if squares is None else squares + one
    half = squares_a.shape[1]
    squares_a[...] = squares[:, :half]
    squares_b[...] = squares[:, half:]


def late_kernel(last, active_total, steps, assign_ref, place_ref, *refs):
    n = len(last)
    scales, got, (flat, squares_ref) = refs[:n], refs[n : 2 * n], refs[2 * n : 2 * n + 2]
    copies = []
    cuts, width = flat.shape
    if steps:
        other_ref, out_ref, out_v, sems = refs[2 * n + 2 :]
        target = out_ref.at[0, pl.ds(0, width)]
        copies.append(pltpu.make_async_copy(other_ref, target, sems.at[steps]))

        def begin(i, carry):
            copies[0].start()
            return carry

        lax.fori_loop(0, jnp.minimum(lax.axis_index("scen") + 1, 1), begin, 0)
    else:
        (out_v,) = refs[2 * n + 2 :]
    squares = squares_ref[...]
    for k, scale, got_ref in zip(last, scales, got):
        squares = squares + place_rows(k, scale[...], got_ref, place_ref, assign_ref, [flat])
    column = jnp.sum(squares, axis=0, keepdims=True)
    inverse = 1.0 / jnp.sqrt(column / active_total + EPS)
    step = 4 * LANES
    for c in range(cuts // step):
        span = pl.ds(c * step, step)
        out_v[:, span] = (flat[span, :] * inverse).T
        if steps:
            target = out_ref.at[0, pl.ds(width, width), span]
            copies.append(pltpu.make_async_copy(out_v.at[:, span], target, sems.at[c]))
            copies[-1].start()
    for one in copies:
        one.wait()


def finish(received, lines_of, totals, place, assign, groups, rows, slice_width):
    cuts = groups * rows
    half = slice_width // 2
    last = halved(groups)
    early = [k for k in range(groups) if k not in last]
    assign = scalars(assign)
    (place,) = on_chip(place)
    flat = pltpu.VMEM((cuts, half), jnp.float32)
    squares = pltpu.VMEM((SUBLANES, half), jnp.float32)
    scale = pltpu.VMEM((ACT_DEV, half), jnp.float32)
    flat_a, flat_b, squares_a, squares_b, *scales = pl.pallas_call(
        functools.partial(
            early_kernel, [(k, lines_of[k]) for k in early], [lines_of[k] for k in last]
        ),
        out_shape=[flat, flat, squares, squares] + [scale] * len(last),
        in_specs=[SMEM] + [VMEM] * (1 + len(totals) + len(early)),
        out_specs=[VMEM] * (4 + len(last)),
        name="early",
        compiler_params=PARAMS,
    )(assign, place, *on_chip(*totals, *[received[k, 0] for k in early]))

    def late(n, flat, squares, *other):
        got = [received[k, n * half // LANES] for k in last]
        values = on_chip(*scales, *got, flat, squares, *other)
        steps = cuts // (4 * LANES) if n else 0
        turned = pltpu.VMEM((half, cuts), jnp.float32)
        whole = jax.ShapeDtypeStruct((1, slice_width, cuts), jnp.float32)
        return pl.pallas_call(
            functools.partial(late_kernel, last, ACT_DEV * groups, steps),
            out_shape=whole if n else turned,
            in_specs=[SMEM] + [VMEM] * (1 + len(values)),
            out_specs=HBM if n else VMEM,
            scratch_shapes=[turned, pltpu.SemaphoreType.DMA((steps + 1,))] if n else [],
            compiler_params=PARAMS,
        )(assign, place, *values)

    return late(1, flat_b, squares_b, late(0, flat_a, squares_a))


def exchange(coef, mask, assign):
    rows, width = coef.shape
    groups = lax.axis_size("scen")
    columns = lax.axis_size("col")
    slice_width = width // groups
    tiles = slice_width // LANES

    def swap(value, k):
        return lax.ppermute(value, "scen", [(i, i ^ k) for i in range(groups)])

    blocks, part = pick(mask, coef, groups, rows, tiles)
    near = evens(groups)
    parts = [part] + [swap(part, k) for k in near[1:]]
    blocks[1, 0] = join(blocks[1, 0], *parts)
    received = {(k, h): swap(block, k) if k else block for (k, h), block in blocks.items()}
    lines = stack(len(near), blocks[1, 0], received[1, 0])
    lines_of = {k: n for n, k in enumerate(near + [k ^ 1 for k in near])}

    def turn(z):
        return lax.ppermute(lines, "col", [(i, (i + z) % columns) for i in range(columns)])

    totals = [lines] + [turn(z) for z in range(1, columns)]
    place, assign = spread(mask, assign, groups, rows)
    return finish(received, lines_of, totals, place, assign, groups, rows, slice_width)


def fallback(coef, mask, assign):
    rows, width = coef.shape
    groups = lax.axis_size("scen")
    slice_width = width // groups
    cut_total = groups * rows
    slot_total = cut_total // K
    active_total = ACT_DEV * groups
    partial_value = jnp.sum(coef * coef, axis=1)
    total = lax.psum(partial_value, "col")
    row_norm = jnp.sqrt(total / NV + EPS)
    device_index = lax.axis_index("scen")
    own_mask = lax.dynamic_slice_in_dim(mask, device_index * rows, rows)
    live = own_mask.astype(jnp.float32)
    scaled = coef / row_norm[:, None] * live[:, None]
    flipped = scaled.T.reshape(groups, slice_width, rows)
    inverse = jnp.argsort(assign, stable=True)
    kept_rows = jnp.argsort(1 - own_mask, stable=True)[:ACT_DEV]
    picked = jnp.take(flipped, kept_rows, axis=2)
    arrived = lax.all_to_all(picked, "scen", split_axis=0, concat_axis=2, tiled=True)
    norm = jnp.sqrt(jnp.sum(arrived * arrived, axis=2, keepdims=True) / active_total + EPS)
    equil = (arrived / norm).reshape(slice_width, groups, ACT_DEV)
    block_masks = mask.reshape(groups, rows)
    chosen = jnp.argsort(1 - block_masks, axis=1, stable=True)[:, :ACT_DEV]
    bundle = min(groups, 8)
    rounds = groups // bundle
    chosen_sets = chosen.reshape(rounds, bundle, ACT_DEV)
    equil_sets = equil.reshape(slice_width, rounds, bundle, ACT_DEV).transpose(1, 0, 2, 3)
    local_rows = jnp.arange(rows, dtype=jnp.int32)

    def place(pair):
        chosen_set, equil_set = pair
        placing = (chosen_set[:, :, None] == local_rows[None, None, :]).astype(jnp.float32)
        return jnp.einsum("sga,gar->sgr", equil_set, placing, precision=lax.Precision.HIGHEST)

    placed = lax.map(place, (chosen_sets, equil_sets))
    whole = placed.transpose(1, 0, 2, 3).reshape(1, slice_width, cut_total)
    slotted = whole.reshape(1, slice_width, slot_total, K)
    return jnp.take(slotted, inverse, axis=2).reshape(1, slice_width, cut_total)


def solution(mesh):
    in_specs = (P("scen", "col"), P(), P())
    out_specs = P("col", "scen", None)
    groups, columns = mesh.shape["scen"], mesh.shape["col"]
    slice_width = NV // (groups * columns)
    fits = groups == 8 and columns == 4 and slice_width % (2 * LANES) == 0
    shard = functools.partial(
        jax.shard_map, mesh=mesh, in_specs=in_specs, out_specs=out_specs, check_vma=False
    )
    if not fits:
        return shard(fallback)
    return shard(exchange)
```

```python
import functools

import jax
import jax.numpy as jnp
from jax import lax
from jax.experimental import pallas as pl
from jax.experimental.pallas import tpu as pltpu
from jax.sharding import PartitionSpec as P

NV = 8192
K = 8
ACT_DEV = 256


EPS = 1e-06
LANES = 128
SUBLANES = 8
VMEM = pl.BlockSpec(memory_space=pltpu.VMEM)
HBM = pl.BlockSpec(memory_space=pltpu.HBM)
SMEM = pl.BlockSpec(memory_space=pltpu.SMEM)
PARAMS = pltpu.CompilerParams(vmem_limit_bytes=16 * 1024 * 1024)


def on_chip(*values):
    return [pltpu.with_memory_space_constraint(value, pltpu.VMEM) for value in values]


def scalars(value):
    return pltpu.with_memory_space_constraint(value, pltpu.SMEM)


def in_hbm(*values):
    return [pltpu.with_memory_space_constraint(value, pltpu.HBM) for value in values]


def evens(groups):
    return list(range(0, groups, 2))


def odds(groups):
    return list(range(1, groups, 2))


def halved(groups):
    return odds(groups)[1:-1]


def pieces(groups, tiles):
    whole = [(k, 0, tiles) for k in range(groups) if k not in halved(groups)]
    first = [(k, 0, tiles // 2) for k in halved(groups)]
    second = [(k, tiles // 2, tiles) for k in halved(groups)]
    return whole + first + second


def ahead_of_all(begin):
    lax.fori_loop(0, jnp.minimum(lax.axis_index("scen") + 1, 1), begin, 0)


def pack(first, picks, window, cells, total):
    lane_row = lax.broadcasted_iota(jnp.int32, (SUBLANES, LANES), 0)
    for t, out, lane in cells:
        tile = window[t, pl.ds(picks[0], SUBLANES), :]
        for j in range(1, SUBLANES):
            tile = jnp.where(lane_row == j, window[t, pl.ds(picks[j], SUBLANES), :], tile)
        out[pl.ds(first, SUBLANES), lane : lane + LANES] = tile
        total = total + tile * tile
    return total


def cells_of(parts, outs, tiles):
    return [
        (k * tiles + h, out, (h - h0) * LANES)
        for (k, h0, h1), out in zip(parts, outs)
        for h in range(h0, h1)
    ]


def first_kernel(groups, rows, tiles, parts, mask_ref, coef_ref, *refs):
    outs = refs[: len(parts)]
    window, squares, order, live, sems, mask_sem = refs[len(parts) :]
    me = lax.axis_index("scen")
    cells = cells_of(parts, outs, tiles)
    ahead = [t for t, _, _ in cells]
    every = groups * tiles
    runs = [(ahead[0], ahead[-1] + 1), (0, ahead[0]), (ahead[-1] + 1, every)]

    def copy(run, t):
        k, h = divmod(t, tiles)
        column = pl.multiple_of((jnp.bitwise_xor(me, k) * tiles + h) * LANES, LANES)
        return pltpu.make_async_copy(
            coef_ref.at[:, pl.ds(column, LANES)], window.at[t, pl.ds(0, rows)], sems.at[run]
        )

    def wait(run):
        start, end = runs[run]
        landed = window.at[pl.ds(start, end - start), pl.ds(0, rows)]
        pltpu.make_async_copy(landed, landed, sems.at[run]).wait()

    mask_copy = pltpu.make_async_copy(mask_ref.at[pl.ds(me * rows, rows)], live, mask_sem)

    def begin(i, carry):
        mask_copy.start()
        return carry

    ahead_of_all(begin)
    for run, (start, end) in enumerate(runs):
        for t in range(start, end):
            copy(run, t).start()

    def note(i, n):
        marks = [live[i * SUBLANES + j] for j in range(SUBLANES)]
        for j in range(SUBLANES):
            order[n] = i * SUBLANES + j
            n = n + marks[j]
        return n

    def gather(i, carry):
        first = pl.multiple_of(i * SUBLANES, SUBLANES)
        picks = [order[first + j] - j for j in range(SUBLANES)]
        total = jnp.zeros((SUBLANES, LANES), jnp.float32)
        squares[pl.ds(first, SUBLANES), :] = pack(first, picks, window, cells, total)
        return carry

    mask_copy.wait()
    lax.fori_loop(0, rows // SUBLANES, note, jnp.int32(0), unroll=4)
    wait(0)
    lax.fori_loop(0, ACT_DEV // SUBLANES, gather, 0, unroll=2)
    wait(1)
    wait(2)


def second_kernel(tiles, parts, window, before, order, *refs):
    outs = refs[: len(parts)]
    part_ref, squares = refs[len(parts) :]
    cells = cells_of(parts, outs, tiles)

    def gather(i, carry):
        first = pl.multiple_of(i * SUBLANES, SUBLANES)
        picks = [order[first + j] - j for j in range(SUBLANES)]
        total = before[pl.ds(first, SUBLANES), :]
        squares[pl.ds(first, SUBLANES), :] = pack(first, picks, window, cells, total)
        return carry

    lax.fori_loop(0, ACT_DEV // SUBLANES, gather, 0)
    part_ref[...] = lax.dot_general(
        jnp.ones((SUBLANES, LANES), jnp.float32), squares[...],
        (((1,), (1,)), ((), ())),
        precision=lax.Precision.HIGHEST, preferred_element_type=jnp.float32,
    )


def pick(mask, coef, groups, rows, tiles):
    parts = pieces(groups, tiles)
    ahead = [part for part in parts if part[0] == evens(groups)[-1]]
    behind = [part for part in parts if part not in ahead]

    def blocks(some):
        room = {1: SUBLANES}
        return [
            pltpu.VMEM((ACT_DEV + room.get(k, 0), (h1 - h0) * LANES), jnp.float32)
            for k, h0, h1 in some
        ]

    squares = pltpu.VMEM((ACT_DEV, LANES), jnp.float32)
    window = pltpu.VMEM((groups * tiles, rows + SUBLANES, LANES), jnp.float32)
    *one, window, before, order = pl.pallas_call(
        functools.partial(first_kernel, groups, rows, tiles, ahead),
        out_shape=blocks(ahead) + [window, squares, pltpu.SMEM((rows,), jnp.int32)],
        in_specs=[HBM, HBM],
        out_specs=[VMEM] * (len(ahead) + 2) + [SMEM],
        scratch_shapes=[
            pltpu.SMEM((rows,), jnp.int32),
            pltpu.SemaphoreType.DMA((3,)),
            pltpu.SemaphoreType.DMA,
        ],
        name="first",
        compiler_params=PARAMS,
    )(*in_hbm(mask, coef))
    *two, part = pl.pallas_call(
        functools.partial(second_kernel, tiles, behind),
        out_shape=blocks(behind) + [pltpu.VMEM((SUBLANES, ACT_DEV), jnp.float32)],
        in_specs=[VMEM, VMEM, SMEM],
        out_specs=[VMEM] * (len(behind) + 1),
        scratch_shapes=[squares],
        name="second",
        compiler_params=PARAMS,
    )(*on_chip(window, before), scalars(order))
    found = zip(ahead + behind, one + two)
    return {(k, h0): block for (k, h0, _), block in found}, part


def join_kernel(block_ref, *refs):
    out_ref = refs[-1]
    for n, ref in enumerate(refs[:-1]):
        out_ref[ACT_DEV + n : ACT_DEV + n + 1, :] = ref[:1, :]


def join(block, *values):
    return pl.pallas_call(
        join_kernel,
        out_shape=pltpu.VMEM(block.shape, jnp.float32),
        in_specs=[VMEM] * (1 + len(values)),
        out_specs=VMEM,
        input_output_aliases={0: 0},
        name="join",
        compiler_params=PARAMS,
    )(*on_chip(block, *values))


def stack_kernel(take, *refs):
    for n, ref in enumerate(refs[:-1]):
        refs[-1][n * take : (n + 1) * take, :] = ref[ACT_DEV : ACT_DEV + take, :]


def stack(take, *values):
    return pl.pallas_call(
        functools.partial(stack_kernel, take),
        out_shape=pltpu.VMEM((take * len(values), values[0].shape[1]), jnp.float32),
        in_specs=[VMEM] * len(values),
        out_specs=VMEM,
        name="stack",
        compiler_params=PARAMS,
    )(*on_chip(*values))


def spread_kernel(groups, rows, mask_ref, assign_ref, place_ref, slots_ref, sem):
    copy = pltpu.make_async_copy(assign_ref, slots_ref, sem)
    copy.start()
    lines = [mask_ref[pl.ds(s * rows, rows)].reshape(1, rows) for s in range(groups)]
    live = jnp.concatenate(lines, axis=0)
    before = lax.broadcasted_iota(jnp.int32, (rows, rows), 0) < lax.broadcasted_iota(
        jnp.int32, (rows, rows), 1
    )
    rank = jnp.dot(
        live.astype(jnp.float32).astype(jnp.bfloat16),
        before.astype(jnp.float32).astype(jnp.bfloat16),
        preferred_element_type=jnp.float32,
    )
    key = jnp.where(live > 0, rank, -1.0).T
    packed = lax.broadcasted_iota(jnp.int32, (rows, ACT_DEV), 1).astype(jnp.float32)
    for s in range(groups):
        hit = key[:, s : s + 1] == packed
        place_ref[s] = jnp.where(hit, 1.0, 0.0).astype(jnp.bfloat16)
    copy.wait()


def spread(mask, assign, groups, rows):
    place = pltpu.VMEM((groups, rows, ACT_DEV), jnp.bfloat16)
    return pl.pallas_call(
        functools.partial(spread_kernel, groups, rows),
        out_shape=[place, pltpu.SMEM(assign.shape, jnp.int32)],
        in_specs=[VMEM, HBM],
        out_specs=[VMEM, SMEM],
        scratch_shapes=[pltpu.SemaphoreType.DMA],
        name="spread",
        compiler_params=PARAMS,
    )(*on_chip(mask), *in_hbm(assign))


def inverse_norms(totals):
    total = totals[0][...]
    for other in totals[1:]:
        total = total + other[...]
    return (1.0 / jnp.sqrt(total / NV + EPS)).T


def place_rows(k, scale, got_ref, place_ref, assign_ref, flats):
    source = jnp.bitwise_xor(lax.axis_index("scen"), k)
    value = got_ref[:ACT_DEV, :] * scale
    high = value.astype(jnp.bfloat16)
    low = (value - high.astype(jnp.float32)).astype(jnp.bfloat16)
    place = place_ref[source]
    both = jnp.concatenate([high, low], axis=1)
    wide = jnp.dot(place, both, preferred_element_type=jnp.float32)
    wide = wide[:, : high.shape[1]] + wide[:, high.shape[1] :]
    slots = wide.shape[0] // K
    for i in range(slots):
        at = pl.multiple_of(assign_ref[source * slots + i] * K, K)
        lane = 0
        for flat in flats:
            width = flat.shape[1]
            flat[pl.ds(at, K), :] = wide[i * K : (i + 1) * K, lane : lane + width]
            lane += width
    return jnp.sum((value * value).reshape(ACT_DEV // SUBLANES, SUBLANES, -1), axis=0)


def early_kernel(lines, rest, assign_ref, place_ref, *refs):
    n = len(lines)
    totals, got = refs[:4], refs[4 : 4 + n]
    outs = refs[4 + n :]
    flats, (squares_a, squares_b), scales = outs[:2], outs[2:4], outs[4:]
    scale = inverse_norms(totals)
    for line, ref in zip(rest, scales):
        ref[...] = jnp.broadcast_to(scale[:, line : line + 1], ref.shape)
    squares = None
    for (k, line), got_ref in zip(lines, got):
        one = place_rows(k, scale[:, line : line + 1], got_ref, place_ref, assign_ref, flats)
        squares = one if squares is None else squares + one
    half = squares_a.shape[1]
    squares_a[...] = squares[:, :half]
    squares_b[...] = squares[:, half:]


def turned_by_matmul(value):
    high = value.astype(jnp.bfloat16)
    low = (value - high.astype(jnp.float32)).astype(jnp.bfloat16)
    both = jnp.concatenate([high, low], axis=1)
    shape = (value.shape[1], both.shape[1])
    row = lax.broadcasted_iota(jnp.int32, shape, 0)
    column = lax.broadcasted_iota(jnp.int32, shape, 1)
    unit = jnp.where(jnp.bitwise_and(column, shape[0] - 1) == row, 1.0, 0.0).astype(jnp.bfloat16)
    return lax.dot_general(
        unit, both, (((1,), (1,)), ((), ())), preferred_element_type=jnp.float32
    )


def late_kernel(last, active_total, half, assign_ref, place_ref, *refs):
    n = len(last)
    scales, got, (flat, squares_ref) = refs[:n], refs[n : 2 * n], refs[2 * n : 2 * n + 2]
    out_ref, out_v, sem = refs[-3:]
    cuts, width = flat.shape
    squares = squares_ref[...]
    for k, scale, got_ref in zip(last, scales, got):
        squares = squares + place_rows(k, scale[...], got_ref, place_ref, assign_ref, [flat])
    column = jnp.sum(squares, axis=0, keepdims=True)
    inverse = 1.0 / jnp.sqrt(column / active_total + EPS)
    step = 4 * LANES
    for c in range(cuts // step):
        span = pl.ds(c * step, step)
        value = flat[span, :] * inverse
        out_v[:, span] = value.T if half or c % 2 == 0 else turned_by_matmul(value)
        target = out_ref.at[0, pl.ds(half * width, width), span]
        pltpu.make_async_copy(out_v.at[:, span], target, sem).start()
    pltpu.make_async_copy(out_v, out_ref.at[0, pl.ds(half * width, width)], sem).wait()


def finish(received, lines_of, totals, place, assign, groups, rows, slice_width):
    cuts = groups * rows
    half = slice_width // 2
    last = halved(groups)
    early = [k for k in range(groups) if k not in last]
    assign = scalars(assign)
    (place,) = on_chip(place)
    flat = pltpu.VMEM((cuts, half), jnp.float32)
    squares = pltpu.VMEM((SUBLANES, half), jnp.float32)
    scale = pltpu.VMEM((ACT_DEV, half), jnp.float32)
    flat_a, flat_b, squares_a, squares_b, *scales = pl.pallas_call(
        functools.partial(
            early_kernel, [(k, lines_of[k]) for k in early], [lines_of[k] for k in last]
        ),
        out_shape=[flat, flat, squares, squares] + [scale] * len(last),
        in_specs=[SMEM] + [VMEM] * (1 + len(totals) + len(early)),
        out_specs=[VMEM] * (4 + len(last)),
        name="early",
        compiler_params=PARAMS,
    )(assign, place, *on_chip(*totals, *[received[k, 0] for k in early]))

    def late(n, flat, squares, *other):
        got = [received[k, n * half // LANES] for k in last]
        values = on_chip(*scales, *got, flat, squares) + in_hbm(*other)
        return pl.pallas_call(
            functools.partial(late_kernel, last, ACT_DEV * groups, n),
            out_shape=jax.ShapeDtypeStruct((1, slice_width, cuts), jnp.float32),
            in_specs=[SMEM] + [VMEM] * (1 + len(values) - n) + [HBM] * n,
            out_specs=HBM,
            scratch_shapes=[pltpu.VMEM((half, cuts), jnp.float32), pltpu.SemaphoreType.DMA],
            input_output_aliases={len(values) + 1: 0} if n else {},
            compiler_params=PARAMS,
        )(assign, place, *values)

    return late(1, flat_b, squares_b, late(0, flat_a, squares_a))


def exchange(coef, mask, assign):
    rows, width = coef.shape
    groups = lax.axis_size("scen")
    columns = lax.axis_size("col")
    slice_width = width // groups
    tiles = slice_width // LANES

    def swap(value, k):
        return lax.ppermute(value, "scen", [(i, i ^ k) for i in range(groups)])

    blocks, part = pick(mask, coef, groups, rows, tiles)
    near = evens(groups)
    parts = [part] + [swap(part, k) for k in near[1:]]
    blocks[1, 0] = join(blocks[1, 0], *parts)
    received = {(k, h): swap(block, k) if k else block for (k, h), block in blocks.items()}
    lines = stack(len(near), blocks[1, 0], received[1, 0])
    lines_of = {k: n for n, k in enumerate(near + [k ^ 1 for k in near])}

    def turn(z):
        return lax.ppermute(lines, "col", [(i, (i + z) % columns) for i in range(columns)])

    totals = [lines] + [turn(z) for z in range(1, columns)]
    place, assign = spread(mask, assign, groups, rows)
    return finish(received, lines_of, totals, place, assign, groups, rows, slice_width)


def fallback(coef, mask, assign):
    rows, width = coef.shape
    groups = lax.axis_size("scen")
    slice_width = width // groups
    cut_total = groups * rows
    slot_total = cut_total // K
    active_total = ACT_DEV * groups
    partial_value = jnp.sum(coef * coef, axis=1)
    total = lax.psum(partial_value, "col")
    row_norm = jnp.sqrt(total / NV + EPS)
    device_index = lax.axis_index("scen")
    own_mask = lax.dynamic_slice_in_dim(mask, device_index * rows, rows)
    live = own_mask.astype(jnp.float32)
    scaled = coef / row_norm[:, None] * live[:, None]
    flipped = scaled.T.reshape(groups, slice_width, rows)
    inverse = jnp.argsort(assign, stable=True)
    kept_rows = jnp.argsort(1 - own_mask, stable=True)[:ACT_DEV]
    picked = jnp.take(flipped, kept_rows, axis=2)
    arrived = lax.all_to_all(picked, "scen", split_axis=0, concat_axis=2, tiled=True)
    norm = jnp.sqrt(jnp.sum(arrived * arrived, axis=2, keepdims=True) / active_total + EPS)
    equil = (arrived / norm).reshape(slice_width, groups, ACT_DEV)
    block_masks = mask.reshape(groups, rows)
    chosen = jnp.argsort(1 - block_masks, axis=1, stable=True)[:, :ACT_DEV]
    bundle = min(groups, 8)
    rounds = groups // bundle
    chosen_sets = chosen.reshape(rounds, bundle, ACT_DEV)
    equil_sets = equil.reshape(slice_width, rounds, bundle, ACT_DEV).transpose(1, 0, 2, 3)
    local_rows = jnp.arange(rows, dtype=jnp.int32)

    def place(pair):
        chosen_set, equil_set = pair
        placing = (chosen_set[:, :, None] == local_rows[None, None, :]).astype(jnp.float32)
        return jnp.einsum("sga,gar->sgr", equil_set, placing, precision=lax.Precision.HIGHEST)

    placed = lax.map(place, (chosen_sets, equil_sets))
    whole = placed.transpose(1, 0, 2, 3).reshape(1, slice_width, cut_total)
    slotted = whole.reshape(1, slice_width, slot_total, K)
    return jnp.take(slotted, inverse, axis=2).reshape(1, slice_width, cut_total)


def solution(mesh):
    in_specs = (P("scen", "col"), P(), P())
    out_specs = P("col", "scen", None)
    groups, columns = mesh.shape["scen"], mesh.shape["col"]
    slice_width = NV // (groups * columns)
    fits = groups == 8 and columns == 4 and slice_width % (2 * LANES) == 0
    shard = functools.partial(
        jax.shard_map, mesh=mesh, in_specs=in_specs, out_specs=out_specs, check_vma=False
    )
    if not fits:
        return shard(fallback)
    return shard(exchange)
```

```python
import functools

import jax
import jax.numpy as jnp
from jax import lax
from jax.experimental import pallas as pl
from jax.experimental.pallas import tpu as pltpu
from jax.sharding import PartitionSpec as P

NV = 8192
K = 8
ACT_DEV = 256


EPS = 1e-06
LANES = 128
SUBLANES = 8
VMEM = pl.BlockSpec(memory_space=pltpu.VMEM)
HBM = pl.BlockSpec(memory_space=pltpu.HBM)
SMEM = pl.BlockSpec(memory_space=pltpu.SMEM)
PARAMS = pltpu.CompilerParams(vmem_limit_bytes=16 * 1024 * 1024)


def on_chip(*values):
    return [pltpu.with_memory_space_constraint(value, pltpu.VMEM) for value in values]


def scalars(value):
    return pltpu.with_memory_space_constraint(value, pltpu.SMEM)


def in_hbm(*values):
    return [pltpu.with_memory_space_constraint(value, pltpu.HBM) for value in values]


def evens(groups):
    return list(range(0, groups, 2))


def odds(groups):
    return list(range(1, groups, 2))


def halved(groups):
    return odds(groups)[1:-1]


def pieces(groups, tiles):
    whole = [(k, 0, tiles) for k in range(groups) if k not in halved(groups)]
    first = [(k, 0, tiles // 2) for k in halved(groups)]
    second = [(k, tiles // 2, tiles) for k in halved(groups)]
    return whole + first + second


def ahead_of_all(begin):
    lax.fori_loop(0, jnp.minimum(lax.axis_index("scen") + 1, 1), begin, 0)


def pack(first, picks, window, cells, total):
    lane_row = lax.broadcasted_iota(jnp.int32, (SUBLANES, LANES), 0)
    for t, out, lane in cells:
        tile = window[t, pl.ds(picks[0], SUBLANES), :]
        for j in range(1, SUBLANES):
            tile = jnp.where(lane_row == j, window[t, pl.ds(picks[j], SUBLANES), :], tile)
        out[pl.ds(first, SUBLANES), lane : lane + LANES] = tile
        total = total + tile * tile
    return total


def cells_of(parts, outs, tiles):
    return [
        (k * tiles + h, out, (h - h0) * LANES)
        for (k, h0, h1), out in zip(parts, outs)
        for h in range(h0, h1)
    ]


def first_kernel(groups, rows, tiles, parts, mask_ref, assign_ref, coef_ref, *refs):
    outs = refs[: len(parts)]
    window, squares, key_ref, order, slots, live, masks, sems, mask_sems = refs[len(parts) :]
    me = lax.axis_index("scen")
    cells = cells_of(parts, outs, tiles)
    ahead = [t for t, _, _ in cells]
    every = groups * tiles
    runs = [(ahead[0], ahead[-1] + 1), (0, ahead[0]), (ahead[-1] + 1, every)]

    def copy(run, t):
        k, h = divmod(t, tiles)
        column = pl.multiple_of((jnp.bitwise_xor(me, k) * tiles + h) * LANES, LANES)
        return pltpu.make_async_copy(
            coef_ref.at[:, pl.ds(column, LANES)], window.at[t, pl.ds(0, rows)], sems.at[run]
        )

    def wait(run):
        start, end = runs[run]
        landed = window.at[pl.ds(start, end - start), pl.ds(0, rows)]
        pltpu.make_async_copy(landed, landed, sems.at[run]).wait()

    small = [
        pltpu.make_async_copy(mask_ref.at[pl.ds(me * rows, rows)], live, mask_sems.at[0]),
        pltpu.make_async_copy(mask_ref, masks, mask_sems.at[1]),
        pltpu.make_async_copy(assign_ref, slots, mask_sems.at[2]),
    ]

    def begin(i, carry):
        for one in small:
            one.start()
        return carry

    ahead_of_all(begin)
    for run, (start, end) in enumerate(runs):
        for t in range(start, end):
            copy(run, t).start()

    def gather(i, carry):
        first = pl.multiple_of(i * SUBLANES, SUBLANES)
        picks = [order[first + j] - j for j in range(SUBLANES)]
        total = jnp.zeros((SUBLANES, LANES), jnp.float32)
        squares[pl.ds(first, SUBLANES), :] = pack(first, picks, window, cells, total)
        return carry

    before = lax.broadcasted_iota(jnp.int32, (rows, rows), 0) < lax.broadcasted_iota(
        jnp.int32, (rows, rows), 1
    )
    before = before.astype(jnp.float32).astype(jnp.bfloat16)
    small[1].wait()
    small[0].wait()
    starts = [pl.multiple_of(jnp.bitwise_xor(me, k) * rows, rows) for k in range(groups)]
    lines = [masks[pl.ds(start, rows)].reshape(1, rows) for start in starts]
    marks = jnp.concatenate(lines, axis=0)
    rank = jnp.dot(
        marks.astype(jnp.float32).astype(jnp.bfloat16),
        before,
        preferred_element_type=jnp.float32,
    )
    n = jnp.int32(0)
    for r in range(rows):
        order[n] = r
        n = n + live[r]
    key_ref[...] = jnp.where(marks > 0, rank, -1.0).T
    wait(0)
    lax.fori_loop(0, ACT_DEV // SUBLANES, gather, 0, unroll=2)
    wait(1)
    wait(2)
    small[2].wait()


def second_kernel(tiles, parts, window, before, order, *refs):
    outs = refs[: len(parts)]
    part_ref, squares = refs[len(parts) :]
    cells = cells_of(parts, outs, tiles)

    def gather(i, carry):
        first = pl.multiple_of(i * SUBLANES, SUBLANES)
        picks = [order[first + j] - j for j in range(SUBLANES)]
        total = before[pl.ds(first, SUBLANES), :]
        squares[pl.ds(first, SUBLANES), :] = pack(first, picks, window, cells, total)
        return carry

    lax.fori_loop(0, ACT_DEV // SUBLANES, gather, 0)
    total = lax.dot_general(
        jnp.ones((SUBLANES, LANES), jnp.float32), squares[...],
        (((1,), (1,)), ((), ())),
        precision=lax.Precision.HIGHEST, preferred_element_type=jnp.float32,
    )
    part_ref[...] = total[:1]


def pick(mask, assign, coef, groups, rows, tiles):
    parts = pieces(groups, tiles)
    ahead = [part for part in parts if part[0] == evens(groups)[-1]]
    behind = [part for part in parts if part not in ahead]

    def blocks(some):
        room = {1: SUBLANES}
        return [
            pltpu.VMEM((ACT_DEV + room.get(k, 0), (h1 - h0) * LANES), jnp.float32)
            for k, h0, h1 in some
        ]

    squares = pltpu.VMEM((ACT_DEV, LANES), jnp.float32)
    window = pltpu.VMEM((groups * tiles, rows + SUBLANES, LANES), jnp.float32)
    key = pltpu.VMEM((rows, groups), jnp.float32)
    listed = [pltpu.SMEM((rows,), jnp.int32), pltpu.SMEM(assign.shape, jnp.int32)]
    *one, window, before, key, order, slots = pl.pallas_call(
        functools.partial(first_kernel, groups, rows, tiles, ahead),
        out_shape=blocks(ahead) + [window, squares, key] + listed,
        in_specs=[HBM, HBM, HBM],
        out_specs=[VMEM] * (len(ahead) + 3) + [SMEM, SMEM],
        scratch_shapes=[
            pltpu.SMEM((rows,), jnp.int32),
            pltpu.VMEM(mask.shape, jnp.int32),
            pltpu.SemaphoreType.DMA((3,)),
            pltpu.SemaphoreType.DMA((3,)),
        ],
        name="first",
        compiler_params=PARAMS,
    )(*in_hbm(mask, assign, coef))
    *two, part = pl.pallas_call(
        functools.partial(second_kernel, tiles, behind),
        out_shape=blocks(behind) + [pltpu.VMEM((1, ACT_DEV), jnp.float32)],
        in_specs=[VMEM, VMEM, SMEM],
        out_specs=[VMEM] * (len(behind) + 1),
        scratch_shapes=[squares],
        name="second",
        compiler_params=PARAMS,
    )(*on_chip(window, before), scalars(order))
    found = zip(ahead + behind, one + two)
    return {(k, h0): block for (k, h0, _), block in found}, part, key, slots


def join_kernel(block_ref, *refs):
    out_ref = refs[-1]
    for n, ref in enumerate(refs[:-1]):
        out_ref[ACT_DEV + n : ACT_DEV + n + 1, :] = ref[:1, :]


def join(block, *values):
    return pl.pallas_call(
        join_kernel,
        out_shape=pltpu.VMEM(block.shape, jnp.float32),
        in_specs=[VMEM] * (1 + len(values)),
        out_specs=VMEM,
        input_output_aliases={0: 0},
        name="join",
        compiler_params=PARAMS,
    )(*on_chip(block, *values))


def stack_kernel(take, *refs):
    for n, ref in enumerate(refs[:-1]):
        refs[-1][n * take : (n + 1) * take, :] = ref[ACT_DEV : ACT_DEV + take, :]


def stack(take, *values):
    return pl.pallas_call(
        functools.partial(stack_kernel, take),
        out_shape=pltpu.VMEM((take * len(values), values[0].shape[1]), jnp.float32),
        in_specs=[VMEM] * len(values),
        out_specs=VMEM,
        name="stack",
        compiler_params=PARAMS,
    )(*on_chip(*values))


def inverse_norms(totals):
    total = totals[0][...]
    for other in totals[1:]:
        total = total + other[...]
    return (1.0 / jnp.sqrt(total / NV + EPS)).T


def matrix(key_ref, k):
    packed = lax.broadcasted_iota(jnp.int32, (key_ref.shape[0], ACT_DEV), 1)
    hit = key_ref[:, k : k + 1] == packed.astype(jnp.float32)
    return jnp.where(hit, 1.0, 0.0).astype(jnp.bfloat16)


def place_rows(k, scale, got_ref, place, assign_ref, flats):
    source = jnp.bitwise_xor(lax.axis_index("scen"), k)
    value = got_ref[:ACT_DEV, :] * scale
    high = value.astype(jnp.bfloat16)
    low = (value - high.astype(jnp.float32)).astype(jnp.bfloat16)
    both = jnp.concatenate([high, low], axis=1)
    wide = jnp.dot(place, both, preferred_element_type=jnp.float32)
    wide = wide[:, : high.shape[1]] + wide[:, high.shape[1] :]
    slots = wide.shape[0] // K
    for i in range(slots):
        at = pl.multiple_of(assign_ref[source * slots + i] * K, K)
        lane = 0
        for flat in flats:
            width = flat.shape[1]
            flat[pl.ds(at, K), :] = wide[i * K : (i + 1) * K, lane : lane + width]
            lane += width
    return jnp.sum((value * value).reshape(ACT_DEV // SUBLANES, SUBLANES, -1), axis=0)


def early_kernel(lines, rest, assign_ref, key_ref, *refs):
    n = len(lines)
    totals, got = refs[:4], refs[4 : 4 + n]
    outs = refs[4 + n :]
    flats, (squares_a, squares_b) = outs[:2], outs[2:4]
    scale = inverse_norms(totals)
    for n, (k, line) in enumerate(rest):
        scale_ref, place_ref = outs[4 + 2 * n : 6 + 2 * n]
        scale_ref[...] = jnp.broadcast_to(scale[:, line : line + 1], scale_ref.shape)
        place_ref[...] = matrix(key_ref, k)
    squares = None
    for (k, line), got_ref in zip(lines, got):
        one = place_rows(
            k, scale[:, line : line + 1], got_ref, matrix(key_ref, k), assign_ref, flats
        )
        squares = one if squares is None else squares + one
    half = squares_a.shape[1]
    squares_a[...] = squares[:, :half]
    squares_b[...] = squares[:, half:]


def turned_by_matmul(value):
    high = value.astype(jnp.bfloat16)
    low = (value - high.astype(jnp.float32)).astype(jnp.bfloat16)
    both = jnp.concatenate([high, low], axis=1)
    shape = (value.shape[1], both.shape[1])
    row = lax.broadcasted_iota(jnp.int32, shape, 0)
    column = lax.broadcasted_iota(jnp.int32, shape, 1)
    unit = jnp.where(jnp.bitwise_and(column, shape[0] - 1) == row, 1.0, 0.0).astype(jnp.bfloat16)
    return lax.dot_general(
        unit, both, (((1,), (1,)), ((), ())), preferred_element_type=jnp.float32
    )


def late_kernel(last, active_total, half, assign_ref, *refs):
    n = len(last)
    scales, places, got = refs[: 2 * n : 2], refs[1 : 2 * n : 2], refs[2 * n : 3 * n]
    flat, squares_ref = refs[3 * n : 3 * n + 2]
    cuts, width = flat.shape
    early = pl.ds(0, cuts // 2)
    late = pl.ds(cuts // 2, cuts // 2)
    own = pl.ds(half * width, width)
    if half:
        other_ref, _, out_ref, out_v, sems = refs[3 * n + 2 :]
        rest = pltpu.make_async_copy(
            other_ref.at[:, late], out_ref.at[0, pl.ds(0, width), late], sems.at[1]
        )

        def begin(i, carry):
            rest.start()
            return carry

        ahead_of_all(begin)
    else:
        out_ref, out_v, sems = refs[3 * n + 2 :]
    squares = squares_ref[...]
    for k, scale, place, got_ref in zip(last, scales, places, got):
        squares = squares + place_rows(k, scale[...], got_ref, place[...], assign_ref, [flat])
    column = jnp.sum(squares, axis=0, keepdims=True)
    inverse = 1.0 / jnp.sqrt(column / active_total + EPS)
    step = 4 * LANES
    for c in range(cuts // step):
        span = pl.ds(c * step, step)
        value = flat[span, :] * inverse
        out_v[:, span] = value.T if half or c % 2 == 0 else turned_by_matmul(value)
        if half or (c + 1) * step <= cuts // 2:
            target = out_ref.at[0, own, span]
            pltpu.make_async_copy(out_v.at[:, span], target, sems.at[0]).start()
    if half:
        rest.wait()
        pltpu.make_async_copy(out_v, out_ref.at[0, own], sems.at[0]).wait()
    else:
        pltpu.make_async_copy(out_v.at[:, early], out_ref.at[0, own, early], sems.at[0]).wait()


def finish(received, lines_of, totals, key, assign, groups, rows, slice_width):
    cuts = groups * rows
    half = slice_width // 2
    last = halved(groups)
    early = [k for k in range(groups) if k not in last]
    assign = scalars(assign)
    flat = pltpu.VMEM((cuts, half), jnp.float32)
    squares = pltpu.VMEM((SUBLANES, half), jnp.float32)
    tables = [pltpu.VMEM((ACT_DEV, half), jnp.float32), pltpu.VMEM((rows, ACT_DEV), jnp.bfloat16)]
    flat_a, flat_b, squares_a, squares_b, *tables = pl.pallas_call(
        functools.partial(
            early_kernel, [(k, lines_of[k]) for k in early], [(k, lines_of[k]) for k in last]
        ),
        out_shape=[flat, flat, squares, squares] + tables * len(last),
        in_specs=[SMEM] + [VMEM] * (1 + len(totals) + len(early)),
        out_specs=[VMEM] * (4 + 2 * len(last)),
        name="early",
        compiler_params=PARAMS,
    )(assign, *on_chip(key, *totals, *[received[k, 0] for k in early]))

    def late(n, flat, squares, *others):
        got = [received[k, n * half // LANES] for k in last]
        values = on_chip(*tables, *got, flat, squares, *others[n:]) + in_hbm(*others[:n])
        whole = jax.ShapeDtypeStruct((1, slice_width, cuts), jnp.float32)
        turned = pltpu.VMEM((half, cuts), jnp.float32)
        return pl.pallas_call(
            functools.partial(late_kernel, last, ACT_DEV * groups, n),
            out_shape=whole if n else [whole, turned],
            in_specs=[SMEM] + [VMEM] * (len(values) - n) + [HBM] * n,
            out_specs=HBM if n else [HBM, VMEM],
            scratch_shapes=[turned] * n + [pltpu.SemaphoreType.DMA((2,))],
            input_output_aliases={len(values): 0} if n else {},
            compiler_params=PARAMS,
        )(assign, *values)

    return late(1, flat_b, squares_b, *late(0, flat_a, squares_a))


def exchange(coef, mask, assign):
    rows, width = coef.shape
    groups = lax.axis_size("scen")
    columns = lax.axis_size("col")
    slice_width = width // groups
    tiles = slice_width // LANES

    def swap(value, k):
        return lax.ppermute(value, "scen", [(i, i ^ k) for i in range(groups)])

    blocks, part, key, slots = pick(mask, assign, coef, groups, rows, tiles)
    near = evens(groups)
    parts = [part] + [swap(part, k) for k in near[1:]]
    blocks[1, 0] = join(blocks[1, 0], *parts)
    received = {(k, h): swap(block, k) if k else block for (k, h), block in blocks.items()}
    lines = stack(len(near), blocks[1, 0], received[1, 0])
    lines_of = {k: n for n, k in enumerate(near + [k ^ 1 for k in near])}

    def turn(z):
        return lax.ppermute(lines, "col", [(i, (i + z) % columns) for i in range(columns)])

    totals = [lines] + [turn(z) for z in range(1, columns)]
    return finish(received, lines_of, totals, key, slots, groups, rows, slice_width)


def fallback(coef, mask, assign):
    rows, width = coef.shape
    groups = lax.axis_size("scen")
    slice_width = width // groups
    cut_total = groups * rows
    slot_total = cut_total // K
    active_total = ACT_DEV * groups
    partial_value = jnp.sum(coef * coef, axis=1)
    total = lax.psum(partial_value, "col")
    row_norm = jnp.sqrt(total / NV + EPS)
    device_index = lax.axis_index("scen")
    own_mask = lax.dynamic_slice_in_dim(mask, device_index * rows, rows)
    live = own_mask.astype(jnp.float32)
    scaled = coef / row_norm[:, None] * live[:, None]
    flipped = scaled.T.reshape(groups, slice_width, rows)
    inverse = jnp.argsort(assign, stable=True)
    kept_rows = jnp.argsort(1 - own_mask, stable=True)[:ACT_DEV]
    picked = jnp.take(flipped, kept_rows, axis=2)
    arrived = lax.all_to_all(picked, "scen", split_axis=0, concat_axis=2, tiled=True)
    norm = jnp.sqrt(jnp.sum(arrived * arrived, axis=2, keepdims=True) / active_total + EPS)
    equil = (arrived / norm).reshape(slice_width, groups, ACT_DEV)
    block_masks = mask.reshape(groups, rows)
    chosen = jnp.argsort(1 - block_masks, axis=1, stable=True)[:, :ACT_DEV]
    bundle = min(groups, 8)
    rounds = groups // bundle
    chosen_sets = chosen.reshape(rounds, bundle, ACT_DEV)
    equil_sets = equil.reshape(slice_width, rounds, bundle, ACT_DEV).transpose(1, 0, 2, 3)
    local_rows = jnp.arange(rows, dtype=jnp.int32)

    def place(pair):
        chosen_set, equil_set = pair
        placing = (chosen_set[:, :, None] == local_rows[None, None, :]).astype(jnp.float32)
        return jnp.einsum("sga,gar->sgr", equil_set, placing, precision=lax.Precision.HIGHEST)

    placed = lax.map(place, (chosen_sets, equil_sets))
    whole = placed.transpose(1, 0, 2, 3).reshape(1, slice_width, cut_total)
    slotted = whole.reshape(1, slice_width, slot_total, K)
    return jnp.take(slotted, inverse, axis=2).reshape(1, slice_width, cut_total)


def solution(mesh):
    in_specs = (P("scen", "col"), P(), P())
    out_specs = P("col", "scen", None)
    groups, columns = mesh.shape["scen"], mesh.shape["col"]
    slice_width = NV // (groups * columns)
    fits = groups == 8 and columns == 4 and slice_width % (2 * LANES) == 0
    shard = functools.partial(
        jax.shard_map, mesh=mesh, in_specs=in_specs, out_specs=out_specs, check_vma=False
    )
    if not fits:
        return shard(fallback)
    return shard(exchange)
```

```python
import functools

import jax
import jax.numpy as jnp
from jax import lax
from jax.experimental import pallas as pl
from jax.experimental.pallas import tpu as pltpu
from jax.sharding import PartitionSpec as P

NV = 8192
K = 8
ACT_DEV = 256


EPS = 1e-06
LANES = 128
SUBLANES = 8
VMEM = pl.BlockSpec(memory_space=pltpu.VMEM)
HBM = pl.BlockSpec(memory_space=pltpu.HBM)
SMEM = pl.BlockSpec(memory_space=pltpu.SMEM)
PARAMS = pltpu.CompilerParams(vmem_limit_bytes=16 * 1024 * 1024)


def on_chip(*values):
    return [pltpu.with_memory_space_constraint(value, pltpu.VMEM) for value in values]


def scalars(value):
    return pltpu.with_memory_space_constraint(value, pltpu.SMEM)


def in_hbm(*values):
    return [pltpu.with_memory_space_constraint(value, pltpu.HBM) for value in values]


def evens(groups):
    return list(range(0, groups, 2))


def odds(groups):
    return list(range(1, groups, 2))


def halved(groups):
    return odds(groups)[1:-1]


def pieces(groups, tiles):
    whole = [(k, 0, tiles) for k in range(groups) if k not in halved(groups)]
    first = [(k, 0, tiles // 2) for k in halved(groups)]
    second = [(k, tiles // 2, tiles) for k in halved(groups)]
    return whole + first + second


def ahead_of_all(begin):
    lax.fori_loop(0, jnp.minimum(lax.axis_index("scen") + 1, 1), begin, 0)


def pack(first, picks, window, cells, total):
    lane_row = lax.broadcasted_iota(jnp.int32, (SUBLANES, LANES), 0)
    for t, out, lane in cells:
        tile = window[t, pl.ds(picks[0], SUBLANES), :]
        for j in range(1, SUBLANES):
            tile = jnp.where(lane_row == j, window[t, pl.ds(picks[j], SUBLANES), :], tile)
        out[pl.ds(first, SUBLANES), lane : lane + LANES] = tile
        total = total + tile * tile
    return total


def cells_of(parts, outs, tiles):
    return [
        (k * tiles + h, out, (h - h0) * LANES)
        for (k, h0, h1), out in zip(parts, outs)
        for h in range(h0, h1)
    ]


def first_kernel(groups, rows, tiles, parts, mask_ref, assign_ref, coef_ref, *refs):
    outs = refs[: len(parts)]
    window, squares, key_ref, order, slots, live, masks, sems, mask_sems = refs[len(parts) :]
    me = lax.axis_index("scen")
    cells = cells_of(parts, outs, tiles)
    ahead = [t for t, _, _ in cells]
    every = groups * tiles
    runs = [(ahead[0], ahead[-1] + 1), (0, ahead[0]), (ahead[-1] + 1, every)]

    def copy(run, t):
        k, h = divmod(t, tiles)
        column = pl.multiple_of((jnp.bitwise_xor(me, k) * tiles + h) * LANES, LANES)
        return pltpu.make_async_copy(
            coef_ref.at[:, pl.ds(column, LANES)], window.at[t, pl.ds(0, rows)], sems.at[run]
        )

    def wait(run):
        start, end = runs[run]
        landed = window.at[pl.ds(start, end - start), pl.ds(0, rows)]
        pltpu.make_async_copy(landed, landed, sems.at[run]).wait()

    small = [
        pltpu.make_async_copy(mask_ref.at[pl.ds(me * rows, rows)], live, mask_sems.at[0]),
        pltpu.make_async_copy(mask_ref, masks, mask_sems.at[1]),
        pltpu.make_async_copy(assign_ref, slots, mask_sems.at[2]),
    ]

    def begin(i, carry):
        for one in small:
            one.start()
        return carry

    ahead_of_all(begin)
    for run, (start, end) in enumerate(runs):
        for t in range(start, end):
            copy(run, t).start()

    def gather(i, carry):
        first = pl.multiple_of(i * SUBLANES, SUBLANES)
        picks = [order[first + j] - j for j in range(SUBLANES)]
        total = jnp.zeros((SUBLANES, LANES), jnp.float32)
        squares[pl.ds(first, SUBLANES), :] = pack(first, picks, window, cells, total)
        return carry

    before = lax.broadcasted_iota(jnp.int32, (rows, rows), 0) < lax.broadcasted_iota(
        jnp.int32, (rows, rows), 1
    )
    before = before.astype(jnp.float32).astype(jnp.bfloat16)
    small[1].wait()
    small[0].wait()
    starts = [pl.multiple_of(jnp.bitwise_xor(me, k) * rows, rows) for k in range(groups)]
    lines = [masks[pl.ds(start, rows)].reshape(1, rows) for start in starts]
    marks = jnp.concatenate(lines, axis=0)
    rank = jnp.dot(
        marks.astype(jnp.float32).astype(jnp.bfloat16),
        before,
        preferred_element_type=jnp.float32,
    )
    n = jnp.int32(0)
    for r in range(rows):
        order[n] = r
        n = n + live[r]
    key_ref[...] = jnp.where(marks > 0, rank, -1.0).T
    wait(0)
    lax.fori_loop(0, ACT_DEV // SUBLANES, gather, 0, unroll=2)
    wait(1)
    wait(2)
    small[2].wait()


def second_kernel(tiles, parts, window, before, order, *refs):
    outs = refs[: len(parts)]
    part_ref, squares = refs[len(parts) :]
    cells = cells_of(parts, outs, tiles)

    def gather(i, carry):
        first = pl.multiple_of(i * SUBLANES, SUBLANES)
        picks = [order[first + j] - j for j in range(SUBLANES)]
        total = before[pl.ds(first, SUBLANES), :]
        squares[pl.ds(first, SUBLANES), :] = pack(first, picks, window, cells, total)
        return carry

    lax.fori_loop(0, ACT_DEV // SUBLANES, gather, 0)
    part_ref[...] = jnp.sum(squares[...].T, axis=0, keepdims=True)


def pick(mask, assign, coef, groups, rows, tiles):
    parts = pieces(groups, tiles)
    ahead = [part for part in parts if part[0] == evens(groups)[-1]]
    behind = [part for part in parts if part not in ahead]

    def blocks(some):
        room = {1: SUBLANES}
        return [
            pltpu.VMEM((ACT_DEV + room.get(k, 0), (h1 - h0) * LANES), jnp.float32)
            for k, h0, h1 in some
        ]

    squares = pltpu.VMEM((ACT_DEV, LANES), jnp.float32)
    window = pltpu.VMEM((groups * tiles, rows + SUBLANES, LANES), jnp.float32)
    key = pltpu.VMEM((rows, groups), jnp.float32)
    listed = [pltpu.SMEM((rows,), jnp.int32), pltpu.SMEM(assign.shape, jnp.int32)]
    *one, window, before, key, order, slots = pl.pallas_call(
        functools.partial(first_kernel, groups, rows, tiles, ahead),
        out_shape=blocks(ahead) + [window, squares, key] + listed,
        in_specs=[HBM, HBM, HBM],
        out_specs=[VMEM] * (len(ahead) + 3) + [SMEM, SMEM],
        scratch_shapes=[
            pltpu.SMEM((rows,), jnp.int32),
            pltpu.VMEM(mask.shape, jnp.int32),
            pltpu.SemaphoreType.DMA((3,)),
            pltpu.SemaphoreType.DMA((3,)),
        ],
        name="first",
        compiler_params=PARAMS,
    )(*in_hbm(mask, assign, coef))
    *two, part = pl.pallas_call(
        functools.partial(second_kernel, tiles, behind),
        out_shape=blocks(behind) + [pltpu.VMEM((1, ACT_DEV), jnp.float32)],
        in_specs=[VMEM, VMEM, SMEM],
        out_specs=[VMEM] * (len(behind) + 1),
        scratch_shapes=[squares],
        name="second",
        compiler_params=PARAMS,
    )(*on_chip(window, before), scalars(order))
    found = zip(ahead + behind, one + two)
    return {(k, h0): block for (k, h0, _), block in found}, part, key, slots


def join_kernel(block_ref, *refs):
    out_ref = refs[-1]
    for n, ref in enumerate(refs[:-1]):
        out_ref[ACT_DEV + n : ACT_DEV + n + 1, :] = ref[:1, :]


def join(block, *values):
    return pl.pallas_call(
        join_kernel,
        out_shape=pltpu.VMEM(block.shape, jnp.float32),
        in_specs=[VMEM] * (1 + len(values)),
        out_specs=VMEM,
        input_output_aliases={0: 0},
        name="join",
        compiler_params=PARAMS,
    )(*on_chip(block, *values))


def stack_kernel(take, *refs):
    for n, ref in enumerate(refs[:-1]):
        refs[-1][n * take : (n + 1) * take, :] = ref[ACT_DEV : ACT_DEV + take, :]


def stack(take, *values):
    return pl.pallas_call(
        functools.partial(stack_kernel, take),
        out_shape=pltpu.VMEM((take * len(values), values[0].shape[1]), jnp.float32),
        in_specs=[VMEM] * len(values),
        out_specs=VMEM,
        name="stack",
        compiler_params=PARAMS,
    )(*on_chip(*values))


def inverse_norms(totals):
    total = totals[0][...]
    for other in totals[1:]:
        total = total + other[...]
    return (1.0 / jnp.sqrt(total / NV + EPS)).T


def matrix(key_ref, k):
    packed = lax.broadcasted_iota(jnp.int32, (key_ref.shape[0], ACT_DEV), 1)
    hit = key_ref[:, k : k + 1] == packed.astype(jnp.float32)
    return jnp.where(hit, 1.0, 0.0).astype(jnp.bfloat16)


def place_rows(k, scale, got_ref, place, assign_ref, flats):
    source = jnp.bitwise_xor(lax.axis_index("scen"), k)
    value = got_ref[:ACT_DEV, :] * scale
    high = value.astype(jnp.bfloat16)
    low = (value - high.astype(jnp.float32)).astype(jnp.bfloat16)
    both = jnp.concatenate([high, low], axis=1)
    wide = jnp.dot(place, both, preferred_element_type=jnp.float32)
    wide = wide[:, : high.shape[1]] + wide[:, high.shape[1] :]
    slots = wide.shape[0] // K
    for i in range(slots):
        at = pl.multiple_of(assign_ref[source * slots + i] * K, K)
        lane = 0
        for flat in flats:
            width = flat.shape[1]
            flat[pl.ds(at, K), :] = wide[i * K : (i + 1) * K, lane : lane + width]
            lane += width
    return jnp.sum((value * value).reshape(ACT_DEV // SUBLANES, SUBLANES, -1), axis=0)


def early_kernel(lines, rest, columns, assign_ref, key_ref, *refs):
    n = len(lines)
    totals, got = refs[:columns], refs[columns : columns + n]
    outs = refs[columns + n :]
    flats, (squares_a, squares_b) = outs[:2], outs[2:4]
    scale = inverse_norms(totals)
    for n, (k, line) in enumerate(rest):
        scale_ref, place_ref = outs[4 + 2 * n : 6 + 2 * n]
        scale_ref[...] = jnp.broadcast_to(scale[:, line : line + 1], scale_ref.shape)
        place_ref[...] = matrix(key_ref, k)
    squares = None
    for (k, line), got_ref in zip(lines, got):
        one = place_rows(
            k, scale[:, line : line + 1], got_ref, matrix(key_ref, k), assign_ref, flats
        )
        squares = one if squares is None else squares + one
    half = squares_a.shape[1]
    squares_a[...] = squares[:, :half]
    squares_b[...] = squares[:, half:]


def turned_by_matmul(value):
    high = value.astype(jnp.bfloat16)
    low = (value - high.astype(jnp.float32)).astype(jnp.bfloat16)
    both = jnp.concatenate([high, low], axis=1)
    shape = (value.shape[1], both.shape[1])
    row = lax.broadcasted_iota(jnp.int32, shape, 0)
    column = lax.broadcasted_iota(jnp.int32, shape, 1)
    unit = jnp.where(jnp.bitwise_and(column, shape[0] - 1) == row, 1.0, 0.0).astype(jnp.bfloat16)
    return lax.dot_general(
        unit, both, (((1,), (1,)), ((), ())), preferred_element_type=jnp.float32
    )


def late_kernel(last, active_total, half, assign_ref, *refs):
    n = len(last)
    scales, places, got = refs[: 2 * n : 2], refs[1 : 2 * n : 2], refs[2 * n : 3 * n]
    flat, squares_ref = refs[3 * n : 3 * n + 2]
    cuts, width = flat.shape
    early = pl.ds(0, cuts // 2)
    late = pl.ds(cuts // 2, cuts // 2)
    own = pl.ds(half * width, width)
    if half:
        other_ref, _, out_ref, out_v, sems = refs[3 * n + 2 :]
        rest = pltpu.make_async_copy(
            other_ref.at[:, late], out_ref.at[0, pl.ds(0, width), late], sems.at[1]
        )

        def begin(i, carry):
            rest.start()
            return carry

        ahead_of_all(begin)
    else:
        out_ref, out_v, sems = refs[3 * n + 2 :]
    squares = squares_ref[...]
    for k, scale, place, got_ref in zip(last, scales, places, got):
        squares = squares + place_rows(k, scale[...], got_ref, place[...], assign_ref, [flat])
    column = jnp.sum(squares, axis=0, keepdims=True)
    inverse = 1.0 / jnp.sqrt(column / active_total + EPS)
    step = 4 * LANES
    for c in range(cuts // step):
        span = pl.ds(c * step, step)
        value = flat[span, :] * inverse
        out_v[:, span] = value.T if half or c % 2 == 0 else turned_by_matmul(value)
        if half or (c + 1) * step <= cuts // 2:
            target = out_ref.at[0, own, span]
            pltpu.make_async_copy(out_v.at[:, span], target, sems.at[0]).start()
    if half:
        rest.wait()
        pltpu.make_async_copy(out_v, out_ref.at[0, own], sems.at[0]).wait()
    else:
        pltpu.make_async_copy(out_v.at[:, early], out_ref.at[0, own, early], sems.at[0]).wait()


def finish(received, lines_of, totals, key, assign, groups, rows, slice_width):
    cuts = groups * rows
    half = slice_width // 2
    last = halved(groups)
    early = [k for k in range(groups) if k not in last]
    assign = scalars(assign)
    flat = pltpu.VMEM((cuts, half), jnp.float32)
    squares = pltpu.VMEM((SUBLANES, half), jnp.float32)
    tables = [pltpu.VMEM((ACT_DEV, half), jnp.float32), pltpu.VMEM((rows, ACT_DEV), jnp.bfloat16)]
    flat_a, flat_b, squares_a, squares_b, *tables = pl.pallas_call(
        functools.partial(
            early_kernel,
            [(k, lines_of[k]) for k in early],
            [(k, lines_of[k]) for k in last],
            len(totals),
        ),
        out_shape=[flat, flat, squares, squares] + tables * len(last),
        in_specs=[SMEM] + [VMEM] * (1 + len(totals) + len(early)),
        out_specs=[VMEM] * (4 + 2 * len(last)),
        name="early",
        compiler_params=PARAMS,
    )(assign, *on_chip(key, *totals, *[received[k, 0] for k in early]))

    def late(n, flat, squares, *others):
        got = [received[k, n * half // LANES] for k in last]
        values = on_chip(*tables, *got, flat, squares, *others[n:]) + in_hbm(*others[:n])
        whole = jax.ShapeDtypeStruct((1, slice_width, cuts), jnp.float32)
        turned = pltpu.VMEM((half, cuts), jnp.float32)
        return pl.pallas_call(
            functools.partial(late_kernel, last, ACT_DEV * groups, n),
            out_shape=whole if n else [whole, turned],
            in_specs=[SMEM] + [VMEM] * (len(values) - n) + [HBM] * n,
            out_specs=HBM if n else [HBM, VMEM],
            scratch_shapes=[turned] * n + [pltpu.SemaphoreType.DMA((2,))],
            input_output_aliases={len(values): 0} if n else {},
            compiler_params=PARAMS,
        )(assign, *values)

    return late(1, flat_b, squares_b, *late(0, flat_a, squares_a))


def exchange(coef, mask, assign):
    rows, width = coef.shape
    groups = lax.axis_size("scen")
    columns = lax.axis_size("col")
    slice_width = width // groups
    tiles = slice_width // LANES

    def swap(value, k):
        return lax.ppermute(value, "scen", [(i, i ^ k) for i in range(groups)])

    blocks, part, key, slots = pick(mask, assign, coef, groups, rows, tiles)
    near = evens(groups)
    parts = [part] + [swap(part, k) for k in near[1:]]
    blocks[1, 0] = join(blocks[1, 0], *parts)
    received = {(k, h): swap(block, k) if k else block for (k, h), block in blocks.items()}
    lines = stack(len(near), blocks[1, 0], received[1, 0])
    lines_of = {k: n for n, k in enumerate(near + [k ^ 1 for k in near])}

    def turn(z):
        return lax.ppermute(lines, "col", [(i, (i + z) % columns) for i in range(columns)])

    totals = [lines] + [turn(z) for z in range(1, columns)]
    return finish(received, lines_of, totals, key, slots, groups, rows, slice_width)


def fallback(coef, mask, assign):
    rows, width = coef.shape
    groups = lax.axis_size("scen")
    slice_width = width // groups
    cut_total = groups * rows
    slot_total = cut_total // K
    active_total = ACT_DEV * groups
    partial_value = jnp.sum(coef * coef, axis=1)
    total = lax.psum(partial_value, "col")
    row_norm = jnp.sqrt(total / NV + EPS)
    device_index = lax.axis_index("scen")
    own_mask = lax.dynamic_slice_in_dim(mask, device_index * rows, rows)
    live = own_mask.astype(jnp.float32)
    scaled = coef / row_norm[:, None] * live[:, None]
    flipped = scaled.T.reshape(groups, slice_width, rows)
    inverse = jnp.argsort(assign, stable=True)
    kept_rows = jnp.argsort(1 - own_mask, stable=True)[:ACT_DEV]
    picked = jnp.take(flipped, kept_rows, axis=2)
    arrived = lax.all_to_all(picked, "scen", split_axis=0, concat_axis=2, tiled=True)
    norm = jnp.sqrt(jnp.sum(arrived * arrived, axis=2, keepdims=True) / active_total + EPS)
    equil = (arrived / norm).reshape(slice_width, groups, ACT_DEV)
    block_masks = mask.reshape(groups, rows)
    chosen = jnp.argsort(1 - block_masks, axis=1, stable=True)[:, :ACT_DEV]
    bundle = min(groups, 8)
    rounds = groups // bundle
    chosen_sets = chosen.reshape(rounds, bundle, ACT_DEV)
    equil_sets = equil.reshape(slice_width, rounds, bundle, ACT_DEV).transpose(1, 0, 2, 3)
    local_rows = jnp.arange(rows, dtype=jnp.int32)

    def place(pair):
        chosen_set, equil_set = pair
        placing = (chosen_set[:, :, None] == local_rows[None, None, :]).astype(jnp.float32)
        return jnp.einsum("sga,gar->sgr", equil_set, placing, precision=lax.Precision.HIGHEST)

    placed = lax.map(place, (chosen_sets, equil_sets))
    whole = placed.transpose(1, 0, 2, 3).reshape(1, slice_width, cut_total)
    slotted = whole.reshape(1, slice_width, slot_total, K)
    return jnp.take(slotted, inverse, axis=2).reshape(1, slice_width, cut_total)


def solution(mesh):
    in_specs = (P("scen", "col"), P(), P())
    out_specs = P("col", "scen", None)
    groups, columns = mesh.shape["scen"], mesh.shape["col"]
    slice_width = NV // (groups * columns)
    fits = groups == 8 and slice_width % (2 * LANES) == 0
    shard = functools.partial(
        jax.shard_map, mesh=mesh, in_specs=in_specs, out_specs=out_specs, check_vma=False
    )
    if not fits:
        return shard(fallback)
    return shard(exchange)
```

```python
import functools

import jax
import jax.numpy as jnp
from jax import lax
from jax.experimental import pallas as pl
from jax.experimental.pallas import tpu as pltpu
from jax.sharding import PartitionSpec as P

NV = 8192
K = 8
ACT_DEV = 256


EPS = 1e-06
LANES = 128
SUBLANES = 8
VMEM = pl.BlockSpec(memory_space=pltpu.VMEM)
HBM = pl.BlockSpec(memory_space=pltpu.HBM)
SMEM = pl.BlockSpec(memory_space=pltpu.SMEM)
PARAMS = pltpu.CompilerParams(vmem_limit_bytes=16 * 1024 * 1024)


def on_chip(*values):
    return [pltpu.with_memory_space_constraint(value, pltpu.VMEM) for value in values]


def scalars(value):
    return pltpu.with_memory_space_constraint(value, pltpu.SMEM)


def in_hbm(*values):
    return [pltpu.with_memory_space_constraint(value, pltpu.HBM) for value in values]


def evens(groups):
    return list(range(0, groups, 2))


def odds(groups):
    return list(range(1, groups, 2))


def halved(groups):
    return odds(groups)[1:-1]


def pieces(groups, tiles):
    whole = [(k, 0, tiles) for k in range(groups) if k not in halved(groups)]
    first = [(k, 0, tiles // 2) for k in halved(groups)]
    second = [(k, tiles // 2, tiles) for k in halved(groups)]
    return whole + first + second


def ahead_of_all(begin):
    lax.fori_loop(0, jnp.minimum(lax.axis_index("scen") + 1, 1), begin, 0)


def pack(first, picks, window, cells, total):
    lane_row = lax.broadcasted_iota(jnp.int32, (SUBLANES, LANES), 0)
    for t, out, lane in cells:
        tile = window[t, pl.ds(picks[0], SUBLANES), :]
        for j in range(1, SUBLANES):
            tile = jnp.where(lane_row == j, window[t, pl.ds(picks[j], SUBLANES), :], tile)
        out[pl.ds(first, SUBLANES), lane : lane + LANES] = tile
        total = total + tile * tile
    return total


def cells_of(parts, outs, tiles):
    return [
        (k * tiles + h, out, (h - h0) * LANES)
        for (k, h0, h1), out in zip(parts, outs)
        for h in range(h0, h1)
    ]


def first_kernel(groups, rows, tiles, parts, mask_ref, assign_ref, coef_ref, *refs):
    outs = refs[: len(parts)]
    squares, key_ref, order, slots, window, live, masks, sems, mask_sems = refs[len(parts) :]
    me = lax.axis_index("scen")
    cells = cells_of(parts, outs, tiles)
    ahead = sorted({t for t, _, _ in cells})
    cells = [(t - ahead[0], out, lane) for t, out, lane in cells]

    def copy(t):
        k, h = divmod(t, tiles)
        column = pl.multiple_of((jnp.bitwise_xor(me, k) * tiles + h) * LANES, LANES)
        return pltpu.make_async_copy(
            coef_ref.at[:, pl.ds(column, LANES)],
            window.at[t - ahead[0], pl.ds(0, rows)],
            sems.at[t - ahead[0]],
        )

    small = [
        pltpu.make_async_copy(mask_ref.at[pl.ds(me * rows, rows)], live, mask_sems.at[0]),
        pltpu.make_async_copy(mask_ref, masks, mask_sems.at[1]),
        pltpu.make_async_copy(assign_ref, slots, mask_sems.at[2]),
    ]

    def begin(i, carry):
        for one in small:
            one.start()
        return carry

    ahead_of_all(begin)
    for t in ahead:
        copy(t).start()

    def gather(i, carry):
        first = pl.multiple_of(i * SUBLANES, SUBLANES)
        picks = [order[first + j] - j for j in range(SUBLANES)]
        total = jnp.zeros((SUBLANES, LANES), jnp.float32)
        squares[pl.ds(first, SUBLANES), :] = pack(first, picks, window, cells, total)
        return carry

    before = lax.broadcasted_iota(jnp.int32, (rows, rows), 0) < lax.broadcasted_iota(
        jnp.int32, (rows, rows), 1
    )
    before = before.astype(jnp.float32).astype(jnp.bfloat16)
    small[1].wait()
    small[0].wait()
    starts = [pl.multiple_of(jnp.bitwise_xor(me, k) * rows, rows) for k in range(groups)]
    lines = [masks[pl.ds(start, rows)].reshape(1, rows) for start in starts]
    marks = jnp.concatenate(lines, axis=0)
    rank = jnp.dot(
        marks.astype(jnp.float32).astype(jnp.bfloat16),
        before,
        preferred_element_type=jnp.float32,
    )
    n = jnp.int32(0)
    for r in range(rows):
        order[n] = r
        n = n + live[r]
    key_ref[...] = jnp.where(marks > 0, rank, -1.0).T
    for t in ahead:
        copy(t).wait()
    lax.fori_loop(0, ACT_DEV // SUBLANES, gather, 0, unroll=2)
    small[2].wait()


def second_kernel(tiles, parts, coef_ref, before, order, *refs):
    outs = refs[: len(parts)]
    part_ref, squares = refs[len(parts) :]
    me = lax.axis_index("scen")
    across = lax.axis_size("scen") * tiles * SUBLANES
    lane_row = lax.broadcasted_iota(jnp.int32, (SUBLANES, LANES), 0)

    def gather(i, carry):
        first = pl.multiple_of(i * SUBLANES, SUBLANES)
        rows_at = [order[first + j] for j in range(SUBLANES)]
        picks = [lax.shift_right_logical(r, 3) * across + jnp.bitwise_and(r, SUBLANES - 1) - j for j, r in enumerate(rows_at)]
        total = before[pl.ds(first, SUBLANES), :]
        for t, out, lane in cells_of(parts, outs, tiles):
            k, h = divmod(t, tiles)
            column = (jnp.bitwise_xor(me, k) * tiles + h) * SUBLANES
            tile = jnp.zeros((SUBLANES, LANES), jnp.float32)
            for j in range(SUBLANES):
                line = coef_ref[pl.ds(picks[j] + column, SUBLANES), :]
                tile = jnp.where(lane_row == j, line, tile)
            out[pl.ds(first, SUBLANES), lane : lane + LANES] = tile
            total = total + tile * tile
        squares[pl.ds(first, SUBLANES), :] = total
        return carry

    lax.fori_loop(0, ACT_DEV // SUBLANES, gather, 0)
    part_ref[...] = jnp.sum(squares[...].T, axis=0, keepdims=True)


def pick(mask, assign, coef, groups, rows, tiles):
    parts = pieces(groups, tiles)
    ahead = [part for part in parts if part[0] == evens(groups)[-1]]
    behind = [part for part in parts if part not in ahead]

    def blocks(some):
        room = {1: SUBLANES}
        return [
            pltpu.VMEM((ACT_DEV + room.get(k, 0), (h1 - h0) * LANES), jnp.float32)
            for k, h0, h1 in some
        ]

    squares = pltpu.VMEM((ACT_DEV, LANES), jnp.float32)
    window = pltpu.VMEM((tiles * len(ahead), rows + SUBLANES, LANES), jnp.float32)
    key = pltpu.VMEM((rows, groups), jnp.float32)
    listed = [pltpu.SMEM((rows,), jnp.int32), pltpu.SMEM(assign.shape, jnp.int32)]
    *one, before, key, order, slots = pl.pallas_call(
        functools.partial(first_kernel, groups, rows, tiles, ahead),
        out_shape=blocks(ahead) + [squares, key] + listed,
        in_specs=[HBM, HBM, HBM],
        out_specs=[VMEM] * (len(ahead) + 2) + [SMEM, SMEM],
        scratch_shapes=[
            window,
            pltpu.SMEM((rows,), jnp.int32),
            pltpu.VMEM(mask.shape, jnp.int32),
            pltpu.SemaphoreType.DMA((3,)),
            pltpu.SemaphoreType.DMA((3,)),
        ],
        name="first",
        compiler_params=PARAMS,
    )(*in_hbm(mask, assign, coef))
    lined = coef.reshape(rows // SUBLANES, SUBLANES, groups * tiles, LANES)
    lined = lined.transpose(0, 2, 1, 3).reshape(-1, LANES)
    *two, part = pl.pallas_call(
        functools.partial(second_kernel, tiles, behind),
        out_shape=blocks(behind) + [pltpu.VMEM((1, ACT_DEV), jnp.float32)],
        in_specs=[VMEM, VMEM, SMEM],
        out_specs=[VMEM] * (len(behind) + 1),
        scratch_shapes=[squares],
        name="second",
        compiler_params=PARAMS,
    )(*on_chip(lined, before), scalars(order))
    found = zip(ahead + behind, one + two)
    return {(k, h0): block for (k, h0, _), block in found}, part, key, slots


def join_kernel(block_ref, *refs):
    out_ref = refs[-1]
    for n, ref in enumerate(refs[:-1]):
        out_ref[ACT_DEV + n : ACT_DEV + n + 1, :] = ref[:1, :]


def join(block, *values):
    return pl.pallas_call(
        join_kernel,
        out_shape=pltpu.VMEM(block.shape, jnp.float32),
        in_specs=[VMEM] * (1 + len(values)),
        out_specs=VMEM,
        input_output_aliases={0: 0},
        name="join",
        compiler_params=PARAMS,
    )(*on_chip(block, *values))


def stack_kernel(take, *refs):
    for n, ref in enumerate(refs[:-1]):
        refs[-1][n * take : (n + 1) * take, :] = ref[ACT_DEV : ACT_DEV + take, :]


def stack(take, *values):
    return pl.pallas_call(
        functools.partial(stack_kernel, take),
        out_shape=pltpu.VMEM((take * len(values), values[0].shape[1]), jnp.float32),
        in_specs=[VMEM] * len(values),
        out_specs=VMEM,
        name="stack",
        compiler_params=PARAMS,
    )(*on_chip(*values))


def inverse_norms(totals):
    total = totals[0][...]
    for other in totals[1:]:
        total = total + other[...]
    return (1.0 / jnp.sqrt(total / NV + EPS)).T


def matrix(key_ref, k):
    packed = lax.broadcasted_iota(jnp.int32, (key_ref.shape[0], ACT_DEV), 1)
    hit = key_ref[:, k : k + 1] == packed.astype(jnp.float32)
    return jnp.where(hit, 1.0, 0.0).astype(jnp.bfloat16)


def place_rows(k, scale, got_ref, place, assign_ref, flats):
    source = jnp.bitwise_xor(lax.axis_index("scen"), k)
    value = got_ref[:ACT_DEV, :] * scale
    high = value.astype(jnp.bfloat16)
    low = (value - high.astype(jnp.float32)).astype(jnp.bfloat16)
    both = jnp.concatenate([high, low], axis=1)
    wide = jnp.dot(place, both, preferred_element_type=jnp.float32)
    wide = wide[:, : high.shape[1]] + wide[:, high.shape[1] :]
    slots = wide.shape[0] // K
    for i in range(slots):
        at = pl.multiple_of(assign_ref[source * slots + i] * K, K)
        lane = 0
        for flat in flats:
            width = flat.shape[1]
            flat[pl.ds(at, K), :] = wide[i * K : (i + 1) * K, lane : lane + width]
            lane += width
    return jnp.sum((value * value).reshape(ACT_DEV // SUBLANES, SUBLANES, -1), axis=0)


def early_kernel(lines, rest, columns, assign_ref, key_ref, *refs):
    n = len(lines)
    totals, got = refs[:columns], refs[columns : columns + n]
    outs = refs[columns + n :]
    flats, (squares_a, squares_b) = outs[:2], outs[2:4]
    scale = inverse_norms(totals)
    for n, (k, line) in enumerate(rest):
        scale_ref, place_ref = outs[4 + 2 * n : 6 + 2 * n]
        scale_ref[...] = jnp.broadcast_to(scale[:, line : line + 1], scale_ref.shape)
        place_ref[...] = matrix(key_ref, k)
    squares = None
    for (k, line), got_ref in zip(lines, got):
        one = place_rows(
            k, scale[:, line : line + 1], got_ref, matrix(key_ref, k), assign_ref, flats
        )
        squares = one if squares is None else squares + one
    half = squares_a.shape[1]
    squares_a[...] = squares[:, :half]
    squares_b[...] = squares[:, half:]


def turned_by_matmul(value):
    high = value.astype(jnp.bfloat16)
    low = (value - high.astype(jnp.float32)).astype(jnp.bfloat16)
    both = jnp.concatenate([high, low], axis=1)
    shape = (value.shape[1], both.shape[1])
    row = lax.broadcasted_iota(jnp.int32, shape, 0)
    column = lax.broadcasted_iota(jnp.int32, shape, 1)
    unit = jnp.where(jnp.bitwise_and(column, shape[0] - 1) == row, 1.0, 0.0).astype(jnp.bfloat16)
    return lax.dot_general(
        unit, both, (((1,), (1,)), ((), ())), preferred_element_type=jnp.float32
    )


def late_kernel(last, active_total, half, assign_ref, *refs):
    n = len(last)
    scales, places, got = refs[: 2 * n : 2], refs[1 : 2 * n : 2], refs[2 * n : 3 * n]
    flat, squares_ref = refs[3 * n : 3 * n + 2]
    cuts, width = flat.shape
    early = pl.ds(0, cuts // 2)
    late = pl.ds(cuts // 2, cuts // 2)
    own = pl.ds(half * width, width)
    if half:
        other_ref, _, out_ref, out_v, sems = refs[3 * n + 2 :]
        rest = pltpu.make_async_copy(
            other_ref.at[:, late], out_ref.at[0, pl.ds(0, width), late], sems.at[1]
        )

        def begin(i, carry):
            rest.start()
            return carry

        ahead_of_all(begin)
    else:
        out_ref, out_v, sems = refs[3 * n + 2 :]
    squares = squares_ref[...]
    for k, scale, place, got_ref in zip(last, scales, places, got):
        squares = squares + place_rows(k, scale[...], got_ref, place[...], assign_ref, [flat])
    column = jnp.sum(squares, axis=0, keepdims=True)
    inverse = 1.0 / jnp.sqrt(column / active_total + EPS)
    step = 4 * LANES
    for c in range(cuts // step):
        span = pl.ds(c * step, step)
        value = flat[span, :] * inverse
        out_v[:, span] = value.T if half or c % 2 == 0 else turned_by_matmul(value)
        if half or (c + 1) * step <= cuts // 2:
            target = out_ref.at[0, own, span]
            pltpu.make_async_copy(out_v.at[:, span], target, sems.at[0]).start()
    if half:
        rest.wait()
        pltpu.make_async_copy(out_v, out_ref.at[0, own], sems.at[0]).wait()
    else:
        pltpu.make_async_copy(out_v.at[:, early], out_ref.at[0, own, early], sems.at[0]).wait()


def finish(received, lines_of, totals, key, assign, groups, rows, slice_width):
    cuts = groups * rows
    half = slice_width // 2
    last = halved(groups)
    early = [k for k in range(groups) if k not in last]
    assign = scalars(assign)
    flat = pltpu.VMEM((cuts, half), jnp.float32)
    squares = pltpu.VMEM((SUBLANES, half), jnp.float32)
    tables = [pltpu.VMEM((ACT_DEV, half), jnp.float32), pltpu.VMEM((rows, ACT_DEV), jnp.bfloat16)]
    flat_a, flat_b, squares_a, squares_b, *tables = pl.pallas_call(
        functools.partial(
            early_kernel,
            [(k, lines_of[k]) for k in early],
            [(k, lines_of[k]) for k in last],
            len(totals),
        ),
        out_shape=[flat, flat, squares, squares] + tables * len(last),
        in_specs=[SMEM] + [VMEM] * (1 + len(totals) + len(early)),
        out_specs=[VMEM] * (4 + 2 * len(last)),
        name="early",
        compiler_params=PARAMS,
    )(assign, *on_chip(key, *totals, *[received[k, 0] for k in early]))

    def late(n, flat, squares, *others):
        got = [received[k, n * half // LANES] for k in last]
        values = on_chip(*tables, *got, flat, squares, *others[n:]) + in_hbm(*others[:n])
        whole = jax.ShapeDtypeStruct((1, slice_width, cuts), jnp.float32)
        turned = pltpu.VMEM((half, cuts), jnp.float32)
        return pl.pallas_call(
            functools.partial(late_kernel, last, ACT_DEV * groups, n),
            out_shape=whole if n else [whole, turned],
            in_specs=[SMEM] + [VMEM] * (len(values) - n) + [HBM] * n,
            out_specs=HBM if n else [HBM, VMEM],
            scratch_shapes=[turned] * n + [pltpu.SemaphoreType.DMA((2,))],
            input_output_aliases={len(values): 0} if n else {},
            compiler_params=PARAMS,
        )(assign, *values)

    return late(1, flat_b, squares_b, *late(0, flat_a, squares_a))


def exchange(coef, mask, assign):
    rows, width = coef.shape
    groups = lax.axis_size("scen")
    columns = lax.axis_size("col")
    slice_width = width // groups
    tiles = slice_width // LANES

    def swap(value, k):
        return lax.ppermute(value, "scen", [(i, i ^ k) for i in range(groups)])

    blocks, part, key, slots = pick(mask, assign, coef, groups, rows, tiles)
    near = evens(groups)
    parts = [part] + [swap(part, k) for k in near[1:]]
    blocks[1, 0] = join(blocks[1, 0], *parts)
    received = {(k, h): swap(block, k) if k else block for (k, h), block in blocks.items()}
    lines = stack(len(near), blocks[1, 0], received[1, 0])
    lines_of = {k: n for n, k in enumerate(near + [k ^ 1 for k in near])}

    def turn(z):
        return lax.ppermute(lines, "col", [(i, (i + z) % columns) for i in range(columns)])

    totals = [lines] + [turn(z) for z in range(1, columns)]
    return finish(received, lines_of, totals, key, slots, groups, rows, slice_width)


def fallback(coef, mask, assign):
    rows, width = coef.shape
    groups = lax.axis_size("scen")
    slice_width = width // groups
    cut_total = groups * rows
    slot_total = cut_total // K
    active_total = ACT_DEV * groups
    partial_value = jnp.sum(coef * coef, axis=1)
    total = lax.psum(partial_value, "col")
    row_norm = jnp.sqrt(total / NV + EPS)
    device_index = lax.axis_index("scen")
    own_mask = lax.dynamic_slice_in_dim(mask, device_index * rows, rows)
    live = own_mask.astype(jnp.float32)
    scaled = coef / row_norm[:, None] * live[:, None]
    flipped = scaled.T.reshape(groups, slice_width, rows)
    inverse = jnp.argsort(assign, stable=True)
    kept_rows = jnp.argsort(1 - own_mask, stable=True)[:ACT_DEV]
    picked = jnp.take(flipped, kept_rows, axis=2)
    arrived = lax.all_to_all(picked, "scen", split_axis=0, concat_axis=2, tiled=True)
    norm = jnp.sqrt(jnp.sum(arrived * arrived, axis=2, keepdims=True) / active_total + EPS)
    equil = (arrived / norm).reshape(slice_width, groups, ACT_DEV)
    block_masks = mask.reshape(groups, rows)
    chosen = jnp.argsort(1 - block_masks, axis=1, stable=True)[:, :ACT_DEV]
    bundle = min(groups, 8)
    rounds = groups // bundle
    chosen_sets = chosen.reshape(rounds, bundle, ACT_DEV)
    equil_sets = equil.reshape(slice_width, rounds, bundle, ACT_DEV).transpose(1, 0, 2, 3)
    local_rows = jnp.arange(rows, dtype=jnp.int32)

    def place(pair):
        chosen_set, equil_set = pair
        placing = (chosen_set[:, :, None] == local_rows[None, None, :]).astype(jnp.float32)
        return jnp.einsum("sga,gar->sgr", equil_set, placing, precision=lax.Precision.HIGHEST)

    placed = lax.map(place, (chosen_sets, equil_sets))
    whole = placed.transpose(1, 0, 2, 3).reshape(1, slice_width, cut_total)
    slotted = whole.reshape(1, slice_width, slot_total, K)
    return jnp.take(slotted, inverse, axis=2).reshape(1, slice_width, cut_total)


def solution(mesh):
    in_specs = (P("scen", "col"), P(), P())
    out_specs = P("col", "scen", None)
    groups, columns = mesh.shape["scen"], mesh.shape["col"]
    slice_width = NV // (groups * columns)
    fits = groups == 8 and slice_width % (2 * LANES) == 0
    shard = functools.partial(
        jax.shard_map, mesh=mesh, in_specs=in_specs, out_specs=out_specs, check_vma=False
    )
    if not fits:
        return shard(fallback)
    return shard(exchange)
```
